256 devices in a mesh: gz: 2 (over core), gx: 16 (over y, x), gy: 8 (over z).
Axes of the slice: x: 4, y: 4, z: 8, core: 2. Of those that a mesh axis runs over, the one named last changes fastest.
Arguments:
- positions: float32 [128, 3, 65536], P(('gz', 'gy'), None, 'gx'), may hold values from -8 to 8
- diffusion_noise: float32 [128, 3, 65536], P(('gz', 'gy'), None, 'gx'), may hold values from -5 to 5
- base_nuclei: float32 [16, 3], replicated, may hold values from -4.15 to 4.15, as said below
- displacements: float32 [8, 16, 3], replicated, may hold values from -0.4375 to 0.4375
- charges: float32 [16], replicated, may hold values from 2 to 14
- orbital_decay: float32 [16], replicated, may hold values from 0.6 to 2
- coefficients: float32 [16], replicated, may hold values from 0.5 to 2
- weights: float32 [65536], P('gx'), may hold values from 0.5 to 2
- counts: int32 [512], P('gx'), may hold values from 1 to 128
- branch_source: int32 [512], replicated, may hold values from 0 to 511, as said below
Outputs:
- local_energy: float32 [8, 65536], P('gz', 'gx')
- energy_estimate: float32 [8], P('gz')
- new_positions: float32 [128, 3, 65536], P(('gz', 'gy'), None, 'gx')
- new_weights: float32 [65536], P('gx')
The draws below stay inside these ranges and needn't reach their ends.
Inputs may be any that keep to these rules, and one draw needn't show every extreme that they name: `branch_source`: A permutation of the blocks. Of the 32 destination blocks of each aligned group (d // 32 equal), at most 4 have sources in any one aligned group of 32 source blocks, and some pair reaches 4 for every group, as sender and as receiver. `base_nuclei`: any two nuclei lie 1.7 or more apart.
All inputs are finite; a program needn't handle non-finite values.
Results may differ from the reference program's by a relative error of at most 0.0002.
Values sent between devices are 32-bit elements; how exact they have to be, the bound alone decides.
No kernel may reach another device: no remote copies, remote signals or barrier semaphores. Data moves between devices by JAX's collectives and lax.ppermute only.
A program may use at most 64 MiB of HBM per device.

```python
import math
import jax
import jax.numpy as jnp
from jax import lax

NE = 128
NA = 16
BLK = 128
G = 8
W = 65536
NBLK = 512
BPD = 32
CAP = 4
N_GX = 16


def draw_base_nuclei(key, part):
    atoms = jnp.arange(NA, dtype=jnp.int32)
    lattice = jnp.stack([atoms % 4, atoms // 4 % 2, atoms // 8], axis=1).astype(jnp.float32) * 2.5
    lattice = lattice - jnp.array([3.75, 1.25, 1.25], dtype=jnp.float32)
    jitter = jax.random.uniform(jax.random.fold_in(key, 11), (NA, 3), jnp.float32, -0.4, 0.4)
    return (lattice + jitter).astype(jnp.float32)


def draw_branch_source(key, part):
    key_sigma = jax.random.fold_in(key, 21)
    key_shift = jax.random.fold_in(key, 22)
    key_order = jax.random.fold_in(key, 23)
    key_slots = jax.random.fold_in(key, 24)
    peers = N_GX
    ranking = jax.random.permutation(key_sigma, peers).astype(jnp.int32) + 3
    ranking = ranking.at[peers // 2].set(0).at[0].set(1).at[1].set(2)
    sigma = jnp.argsort(ranking, stable=True).astype(jnp.int32)
    sigma_inverse = jnp.argsort(sigma).astype(jnp.int32)
    offsets = jnp.arange(peers, dtype=jnp.int32)
    filled = BPD // CAP
    amounts = jnp.where(offsets < filled, CAP, 0).astype(jnp.int32)
    if filled >= 2 and filled < peers:
        moving = jax.random.randint(key_shift, (), 0, CAP).astype(jnp.int32)
        amounts = amounts.at[filled - 1].add(-moving).at[filled].add(moving)
    offset_list = jnp.repeat(offsets, amounts, total_repeat_length=BPD)
    source_device = jnp.broadcast_to(offsets[:, None], (peers, BPD))
    destination = sigma[(sigma_inverse[source_device] + 1 + offset_list[None, :]) % peers]
    local_order = jax.vmap(lambda part_key: jax.random.permutation(part_key, BPD))(jax.random.split(key_order, peers)).astype(jnp.int32)
    source_block = source_device * BPD + local_order
    sort_keys = destination * NBLK + jax.random.permutation(key_slots, NBLK).astype(jnp.int32).reshape(peers, BPD)
    ordering = jnp.argsort(sort_keys.reshape(-1), stable=True)
    return source_block.reshape(-1)[ordering].astype(jnp.int32)


def plant(entries, own_key, least, top_value):
    longest = entries.shape.index(max(entries.shape))
    spots = []
    for shift in (0, 1):
        where = [jax.random.randint(jax.random.fold_in(own_key, axis), (), 0, length) for axis, length in enumerate(entries.shape)]
        where[longest] = (where[longest] + shift) % entries.shape[longest]
        spots.append(tuple(where))
    return entries.at[spots[0]].set(least).at[spots[1]].set(top_value)


def block_levels(own_key, extent, cuts, least, largest):
    loudness = 1.0
    for axis_at, shards_of in cuts:
        draws = jax.random.uniform(jax.random.fold_in(jax.random.fold_in(own_key, 6), axis_at), (shards_of,), jnp.float32, least / len(cuts), largest / len(cuts))
        loudness = loudness * jnp.repeat(jnp.exp(draws), extent[axis_at] // shards_of).reshape((-1,) + (1,) * (len(extent) - 1 - axis_at))
    return loudness


def normal_values(key, extent, spread, bound, cuts=(), kind=jnp.bfloat16):
    result = spread * jax.random.normal(key, extent, jnp.float32)
    if cuts:
        result = result * block_levels(key, extent, cuts, -0.22, 0.18)
    return jnp.clip(result, -bound, bound).astype(kind)


def setup_inputs(seed: int = 0) -> dict:
    streams_of = jax.random.split(jax.random.key(seed), 11)
    positions = normal_values(streams_of[0], (NE, 3, W), 2.0, 8.0, ((0, 16), (2, 16)), jnp.float32)
    diffusion_noise = normal_values(streams_of[1], (NE, 3, W), 1.0, 5.0, ((0, 16), (2, 16)), jnp.float32)
    base_nuclei = draw_base_nuclei(jax.random.fold_in(streams_of[10], 71), 0)
    displacements = normal_values(streams_of[3], (G, NA, 3), 0.03, 0.4375, (), jnp.float32)
    charges = jnp.clip(jnp.exp(jax.random.uniform(streams_of[4], (NA,), jnp.float32, math.log(2.0), math.log(14.0))), 2.0, 14.0)
    orbital_decay = jnp.clip(jnp.exp(jax.random.uniform(streams_of[5], (NA,), jnp.float32, math.log(0.6), math.log(2.0))), 0.6, 2.0)
    coefficients = jnp.clip(jnp.exp(jax.random.uniform(streams_of[6], (NA,), jnp.float32, math.log(0.5), math.log(2.0))), 0.5, 2.0)
    weights = jnp.clip(jnp.exp(math.log(2.0) - 1.3862944 * jax.random.uniform(streams_of[7], (W,), jnp.float32) ** block_levels(streams_of[7], (W,), ((0, 16),), -0.2, 0.2)), 0.5, 2.0)
    counts = plant(jax.random.randint(streams_of[8], (NBLK,), 1, BLK + 1), jax.random.fold_in(streams_of[8], 1), 1, BLK).astype(jnp.int32)
    branch_source = draw_branch_source(jax.random.fold_in(streams_of[10], 71), 0)
    return dict(positions=positions, diffusion_noise=diffusion_noise, base_nuclei=base_nuclei, displacements=displacements, charges=charges, orbital_decay=orbital_decay, coefficients=coefficients, weights=weights, counts=counts, branch_source=branch_source)


soft_square = 0.04
cusp_value = 0.5
jastrow_range = 1.0
time_step = 0.01
step_root = 0.1

def orbital_terms(coords, centers, charges, orbital_decay, coefficients):
    offsets = coords[:, None, :, :] - centers[None, :, :, None]
    square_dist = lax.optimization_barrier(jnp.sum(offsets * offsets, axis=2))
    distance = jnp.sqrt(square_dist + soft_square)
    decay = orbital_decay[None, :, None]
    orbital_part = coefficients[None, :, None] * jnp.exp(-decay * distance)
    orbital = lax.optimization_barrier(jnp.sum(orbital_part, axis=1))
    grad_orbital = lax.optimization_barrier(jnp.sum((-decay * orbital_part / distance)[:, :, None, :] * offsets, axis=1))
    lap_orbital = lax.optimization_barrier(jnp.sum(orbital_part * (decay * decay * square_dist / (distance * distance) - decay * (2.0 * distance * distance + soft_square) / (distance * distance * distance)), axis=1))
    grad_log = grad_orbital / orbital[:, None, :]
    potential = -lax.optimization_barrier(jnp.sum(charges[None, :, None] / distance, axis=1))
    return (jnp.log(orbital), grad_log, lap_orbital / orbital, potential)

def pair_terms(coords, others, coord_index, other_index):
    offsets = coords[:, None, :, :] - others[None, :, :, :]
    square_dist = lax.optimization_barrier(jnp.sum(offsets * offsets, axis=2))
    distance = jnp.sqrt(square_dist + soft_square)
    keeping = (coord_index[:, None] != other_index[None, :]).astype(jnp.float32)[:, :, None]
    denominator = 1.0 + jastrow_range * distance
    slope = keeping * cusp_value / (denominator * denominator)
    bending = keeping * (-2.0 * cusp_value * jastrow_range) / (denominator * denominator * denominator)
    gradient = lax.optimization_barrier(jnp.sum((slope / distance)[:, :, None, :] * offsets, axis=1))
    laplacian = lax.optimization_barrier(jnp.sum(bending * square_dist / (distance * distance) + slope * (2.0 * distance * distance + soft_square) / (distance * distance * distance), axis=1))
    coulomb = 0.5 * lax.optimization_barrier(jnp.sum(keeping / distance, axis=1))
    return (gradient, laplacian, coulomb)

def nuclear_repulsion(centers, charges):
    offsets = centers[:, None, :] - centers[None, :, :]
    identity = jnp.eye(centers.shape[0], dtype=jnp.float32)
    distance = jnp.sqrt(lax.optimization_barrier(jnp.sum(offsets * offsets, axis=2)) + identity)
    return 0.5 * jnp.sum(charges[:, None] * charges[None, :] * (1.0 - identity) / distance)

def electron_energy(grad_log, laplace_ratio, potential, jgrad, jlap, coulomb):
    total_grad = grad_log + jgrad
    kinetic = -0.5 * (laplace_ratio - lax.optimization_barrier(jnp.sum(grad_log * grad_log, axis=1)) + jlap + lax.optimization_barrier(jnp.sum(total_grad * total_grad, axis=1)))
    return kinetic + potential + coulomb

def reference(positions, diffusion_noise, base_nuclei, displacements, charges, orbital_decay, coefficients, weights, counts, branch_source):
    centers = base_nuclei[None, :, :] + displacements
    block_coords = positions.reshape(NE, 3, NBLK, BLK).transpose(2, 0, 1, 3)
    electron_index = jnp.arange(NE, dtype=jnp.int32)

    def walker_block(coords):
        jgrad, jlap, coulomb = pair_terms(coords, coords, electron_index, electron_index)
        energies = []
        log_sums = []
        drifted = coords
        for geometry in range(G):
            log_orbital, grad_log, laplace_ratio, potential = orbital_terms(coords, centers[geometry], charges, orbital_decay, coefficients)
            energies.append(lax.optimization_barrier(jnp.sum(electron_energy(grad_log, laplace_ratio, potential, jgrad, jlap, coulomb), axis=0)))
            log_sums.append(lax.optimization_barrier(jnp.sum(log_orbital, axis=0)))
            if geometry == 0:
                drifted = coords + time_step * (grad_log + jgrad)
        return (jnp.stack(energies), jnp.stack(log_sums), drifted)
    energy_blocks, log_blocks, drift_blocks = lax.map(walker_block, block_coords)
    energies = energy_blocks.transpose(1, 0, 2).reshape(G, W)
    log_sums = log_blocks.transpose(1, 0, 2).reshape(G, W)
    drifted = drift_blocks.transpose(1, 2, 0, 3).reshape(NE, 3, W)
    nuclear_energy = jnp.stack([nuclear_repulsion(centers[geometry], charges) for geometry in range(G)])
    local_energy = (energies + nuclear_energy[:, None]) / NE
    alive_mask = (jnp.arange(BLK, dtype=jnp.int32)[None, :] < counts[:, None]).astype(jnp.float32).reshape(W)
    weight_ratio = jnp.exp(2.0 * (log_sums - log_sums[0:1]))
    sample_weight = weights[None, :] * weight_ratio * alive_mask[None, :]
    energy_estimate = lax.optimization_barrier(jnp.sum(sample_weight * local_energy, axis=1)) / lax.optimization_barrier(jnp.sum(sample_weight, axis=1))
    kept_weights = alive_mask * weights * jnp.exp(-(local_energy[0] - energy_estimate[0]))
    moved_positions = drifted + step_root * diffusion_noise
    new_positions = moved_positions.reshape(NE, 3, NBLK, BLK)[:, :, branch_source].reshape(NE, 3, W)
    new_weights = kept_weights.reshape(NBLK, BLK)[branch_source].reshape(W)
    return (local_energy, energy_estimate, new_positions, new_weights)
```

```python
import functools
import math

import jax
import jax.numpy as jnp
from jax import lax
from jax.experimental import pallas as pl
from jax.experimental.pallas import tpu as pltpu
from jax.sharding import Mesh
from jax.sharding import PartitionSpec as P

NE = 128
NA = 16
NG = 8
BLK = 128
EB = 16
CAP = 4
SLOT_ROWS = 24
PEER_ROWS = CAP * SLOT_ROWS + 8
GX = ("gx_0", "gx_1")
GZY = ("gz", "gy")

SOFT = 0.04
TIME_STEP = 0.01
STEP_ROOT = 0.1
LN2 = math.log(2.0)
LOG2E = 1.0 / LN2

K_CONST, K_X, K_Y, K_Z, K_R2, K_AMP, K_PHI, K_CX, K_CY, K_CZ, K_SOFT, K_POT = range(12)


def roll8(x, shift):
    shift %= 8
    return x if shift == 0 else pltpu.roll(x, shift, axis=0)


def pair_part(pos, rot, back, grad):
    zero = jnp.zeros((8, BLK), jnp.float32)

    def prepare(p, _):
        for h in range(2):
            for c in range(3):
                x = pos[p, h, c * 8 : c * 8 + 8, :]
                grad[p, h, c * 8 : c * 8 + 8, :] = zero
                for s in range(8):
                    rot[p, h, s, c * 8 : c * 8 + 8, :] = roll8(x, -s)
                    back[p, h, s, c * 8 : c * 8 + 8, :] = zero
        return 0

    lax.fori_loop(0, EB, prepare, 0)

    def terms(xi, xj, sums, half):
        d = [xi[c] - xj[c] for c in range(3)]
        square = (d[0] * d[0] + d[1] * d[1]) + (d[2] * d[2] + SOFT)
        inv = lax.rsqrt(square)
        p = 1.0 / (square * inv + 1.0)
        p2 = p * p
        slope = (0.5 * p2) * inv
        p3 = p2 * p
        first = p + p2 + p3
        second = (inv * inv) * (p3 + slope)
        if half:
            first, second = 0.5 * first, 0.5 * second
        return [slope * d[c] for c in range(3)], (sums[0] + first, sums[1] + second)

    def load3(ref, *at):
        return [ref[(*at, slice(c * 8, c * 8 + 8), slice(None))] for c in range(3)]

    def store3(ref, values, *at):
        for c in range(3):
            ref[(*at, slice(c * 8, c * 8 + 8), slice(None))] = values[c]

    def block_pair(i, j, h, xi, gi, sums):
        for s in range(8):
            f, sums = terms(xi, load3(rot, j, h, s), sums, False)
            gi = [gi[c] + f[c] for c in range(3)]
            b = load3(back, j, h, s)
            store3(back, [b[c] + f[c] for c in range(3)], j, h, s)
        return gi, sums

    def inside(t, sums):
        out = []
        for h in range(2):
            acc = sums[h]
            for i in (2 * t, 2 * t + 1):
                xi, gi = load3(pos, i, h), load3(grad, i, h)
                for s in range(1, 5):
                    f, acc = terms(xi, load3(rot, i, h, s), acc, s == 4)
                    gi = [gi[c] + f[c] for c in range(3)]
                    if s < 4:
                        b = load3(back, i, h, s)
                        store3(back, [b[c] + f[c] for c in range(3)], i, h, s)
                store3(grad, gi, i, h)
            i, j = 2 * t, 2 * t + 1
            gi, acc = block_pair(i, j, h, load3(pos, i, h), load3(grad, i, h), acc)
            store3(grad, gi, i, h)
            out.append(acc)
        return tuple(out)

    def across(u, t, sums):
        out = []
        for h in range(2):
            acc = sums[h]
            for i in (2 * u, 2 * u + 1):
                xi, gi = load3(pos, i, h), load3(grad, i, h)
                for j in (2 * t, 2 * t + 1):
                    gi, acc = block_pair(i, j, h, xi, gi, acc)
                store3(grad, gi, i, h)
            out.append(acc)
        return tuple(out)

    def outer(t, sums):
        sums = inside(t, sums)
        return lax.fori_loop(0, t, lambda u, carry: across(u, t, carry), sums)

    start = ((zero, zero), (zero, zero))
    sums = lax.fori_loop(0, EB // 2, outer, start)

    def finish(p, squares):
        out = []
        for h in range(2):
            acc = squares[h]
            for c in range(3):
                g = grad[p, h, c * 8 : c * 8 + 8, :]
                for s in range(8):
                    g = g - roll8(back[p, h, s, c * 8 : c * 8 + 8, :], s)
                grad[p, h, c * 8 : c * 8 + 8, :] = g
                acc = acc + g * g
            out.append(acc)
        return tuple(out)

    squares = lax.fori_loop(0, EB, finish, (zero, zero))
    totals = []
    for h in range(2):
        t = sums[h][0] - SOFT * sums[h][1] - 0.5 * squares[h]
        totals.append(jnp.broadcast_to(jnp.sum(t, axis=0, keepdims=True), (8, BLK)))
    return totals


def walker_kernel(pos, table, nuclear, live, out, rot, back, grad):
    totals = pair_part(pos, rot, back, grad)
    zero = jnp.zeros((8, BLK), jnp.float32)

    def electrons(p, carry):
        energy, logs, pots = carry
        for e in range(8):
            xs, acc = [], []
            for h in range(2):
                x = [
                    jnp.broadcast_to(pos[p, h, c * 8 + e : c * 8 + e + 1, :], (8, BLK))
                    for c in range(3)
                ]
                xs.append((x[0], x[1], x[2], x[0] * x[0] + x[1] * x[1] + x[2] * x[2]))
                acc.append([zero] * 7)
            pots = list(pots)
            for a in range(NA):
                for h in range(2):
                    x, y, z, r2 = xs[h]
                    square = (r2 * table[K_R2, a] + table[K_CONST, a]) + (
                        (x * table[K_X, a] + y * table[K_Y, a]) + z * table[K_Z, a]
                    )
                    inv = lax.rsqrt(square)
                    amp = jnp.exp2(table[K_AMP, a] - square * inv)
                    u = amp * inv
                    s = acc[h]
                    acc[h] = [
                        s[0] + amp * table[K_PHI, a],
                        s[1] + amp,
                        s[2] + u,
                        s[3] + u * table[K_CX, a],
                        s[4] + u * table[K_CY, a],
                        s[5] + u * table[K_CZ, a],
                        s[6] + (u * inv) * ((inv + LN2) * table[K_SOFT, a]),
                    ]
                    pots[h] = pots[h] + inv * table[K_POT, a]
            new_energy, new_logs = [], []
            for h in range(2):
                phi, amps, us, ux, uy, uz, soft = acc[h]
                x, y, z, _ = xs[h]
                ratio = 1.0 / phi
                g = [(ux - x * us) * ratio, (uy - y * us) * ratio, (uz - z * us) * ratio]
                j = [
                    jnp.broadcast_to(grad[p, h, c * 8 + e : c * 8 + e + 1, :], (8, BLK))
                    for c in range(3)
                ]
                lap = (LN2 * amps - 2.0 * us - soft) * ratio
                dot = g[0] * j[0] + g[1] * j[1] + g[2] * j[2]
                new_energy.append(energy[h] - (0.5 * lap + dot))
                new_logs.append(logs[h] + jnp.log2(phi))
                for c in range(3):
                    out[p, h, c * 8 + e : c * 8 + e + 1, :] = (g[c] + j[c])[0:1, :]
            energy, logs = new_energy, new_logs
        return tuple(energy), tuple(logs), tuple(pots)

    energy, logs, pots = lax.fori_loop(
        0, EB, electrons, ((zero, zero), (zero, zero), (zero, zero))
    )
    row = lax.broadcasted_iota(jnp.int32, (8, BLK), 0)
    lane = lax.broadcasted_iota(jnp.int32, (8, BLK), 1)
    numerator = jnp.zeros((8, 1), jnp.float32)
    denominator = jnp.zeros((8, 1), jnp.float32)
    local = []
    for h in range(2):
        e = (energy[h] - pots[h] + totals[h] + nuclear[...]) * (1.0 / NE)
        weight = jnp.exp2(2.0 * (logs[h] - jnp.broadcast_to(logs[h][0:1, :], (8, BLK))))
        weight = weight * jnp.broadcast_to(live[h : h + 1, :], (8, BLK))
        numerator = numerator + jnp.sum(weight * e, axis=1, keepdims=True)
        denominator = denominator + jnp.sum(weight, axis=1, keepdims=True)
        local.append(e)
    placed = jnp.where(lane == row, numerator, 0.0) + jnp.where(lane == row + 8, denominator, 0.0)
    placed = jnp.broadcast_to(jnp.sum(placed, axis=0, keepdims=True), (8, BLK))
    for h in range(2):
        first = jnp.broadcast_to(local[h][0:1, :], (8, BLK))
        for half in range(2):
            e = local[h] if half == 0 else roll8(local[h], 4)
            tile = jnp.where(row < 4, e, jnp.where(row == 4, first, placed))
            for q in range(8):
                out[half * 8 + q, h, 24:32, :] = tile


def walker_step(whole, table, nuclear, live):
    vmem = pl.BlockSpec(memory_space=pltpu.VMEM)
    return pl.pallas_call(
        walker_kernel,
        out_shape=jax.ShapeDtypeStruct((EB, 2, 32, BLK), jnp.float32),
        in_specs=[vmem] * 4,
        out_specs=vmem,
        scratch_shapes=[
            pltpu.VMEM((EB, 2, 8, 24, BLK), jnp.float32),
            pltpu.VMEM((EB, 2, 8, 24, BLK), jnp.float32),
            pltpu.VMEM((EB, 2, 24, BLK), jnp.float32),
        ],
        name="walker_step",
    )(whole, table, nuclear, live)


def pack_kernel(picked, returned, base, live, send, energy):
    sums = returned[0, 29:30, :]
    for p in range(1, EB):
        sums = sums + returned[2 * p, 29:30, :]
    for b in range(2 * EB):
        energy[:, b * BLK : (b + 1) * BLK] = returned[b, 24:28, :]

    def one_peer(peer, _):
        for k in range(CAP):
            b = picked[peer * CAP + k]
            for c in range(3):
                send[peer, k * 24 + c * 8 : k * 24 + c * 8 + 8, :] = (
                    base[b, c * 8 : c * 8 + 8, :] + TIME_STEP * returned[b, c * 8 : c * 8 + 8, :]
                )
            alive = live[pl.ds(b, 1), :]
            level = returned[b, 28:29, :] - jnp.log(alive)
            send[peer, 96 + k : 97 + k, :] = jnp.where(alive > 0.0, level, 3.0e38)
        send[peer, 100:101, :] = sums
        send[peer, 101:104, :] = jnp.zeros((3, BLK), jnp.float32)
        return 0

    lax.fori_loop(0, send.shape[0], one_peer, 0)


def pack_step(picked, returned, base, live, peers):
    vmem = pl.BlockSpec(memory_space=pltpu.VMEM)
    return pl.pallas_call(
        pack_kernel,
        out_shape=(
            jax.ShapeDtypeStruct((peers, PEER_ROWS, BLK), jnp.float32),
            jax.ShapeDtypeStruct((NG // 2, 2 * EB * BLK), jnp.float32),
        ),
        in_specs=[pl.BlockSpec(memory_space=pltpu.SMEM)] + [vmem] * 3,
        out_specs=(vmem, vmem),
        name="pack_step",
    )(picked, returned, base, live)


def place_kernel(slots, half, received, moved, weights, estimate):
    sums = received[0, 100:101, :]
    for peer in range(1, received.shape[0]):
        sums = sums + received[peer, 100:101, :]
    sums = jnp.broadcast_to(sums, (8, BLK))
    ratio = sums / pltpu.roll(sums, BLK - 8, axis=1)
    lane = lax.broadcasted_iota(jnp.int32, (8, BLK), 1)
    reference = jnp.sum(jnp.where(lane == 0, ratio, 0.0), axis=1, keepdims=True)[0:1, :]
    own = jnp.where(half[0] == 0, ratio, pltpu.roll(ratio, BLK - 4, axis=1))
    estimate[...] = own[0:1, 0:4]
    for d in range(weights.shape[0]):
        peer, k = slots[d] // CAP, slots[d] % CAP
        for e in range(8):
            rows = [received[peer, pl.ds(k * 24 + c * 8 + e, 1), :] for c in range(3)]
            for c in range(3):
                moved[e, c : c + 1, d * BLK : (d + 1) * BLK] = rows[c]
        level = received[peer, pl.ds(96 + k, 1), :]
        weights[d : d + 1, :] = jnp.exp(-(level - reference))


def place_step(slots, half, received):
    vmem = pl.BlockSpec(memory_space=pltpu.VMEM)
    smem = pl.BlockSpec(memory_space=pltpu.SMEM)
    blocks = slots.shape[0]
    return pl.pallas_call(
        place_kernel,
        out_shape=(
            jax.ShapeDtypeStruct((8, 3, blocks * BLK), jnp.float32),
            jax.ShapeDtypeStruct((blocks, BLK), jnp.float32),
            jax.ShapeDtypeStruct((1, NG // 2), jnp.float32),
        ),
        in_specs=[smem, smem, vmem],
        out_specs=(vmem, vmem, vmem),
        name="place_step",
    )(slots, half, received)


def nuclear_repulsion(centers, charges):
    offsets = centers[:, :, None, :] - centers[:, None, :, :]
    identity = jnp.eye(NA, dtype=jnp.float32)
    distance = jnp.sqrt(jnp.sum(offsets * offsets, axis=3) + identity)
    product = charges[:, None] * charges[None, :] * (1.0 - identity)
    return 0.5 * jnp.sum(product / distance, axis=(1, 2))


def nucleus_table(centers, charges, decay, coefficients):
    c = jnp.moveaxis(centers, 1, 0)
    k = (decay * LOG2E)[:, None]
    k2 = k * k
    scale = decay[:, None] * k
    ones = jnp.ones((NA, NG), jnp.float32)
    rows = [
        k2 * (jnp.sum(c * c, axis=2) + SOFT),
        -2.0 * k2 * c[:, :, 0],
        -2.0 * k2 * c[:, :, 1],
        -2.0 * k2 * c[:, :, 2],
        k2 * ones,
        jnp.log2(coefficients[:, None] * scale) * ones,
        ones / scale,
        c[:, :, 0],
        c[:, :, 1],
        c[:, :, 2],
        SOFT * k2 * ones,
        (charges[:, None] * k) * ones,
    ]
    return jnp.broadcast_to(jnp.stack(rows)[..., None], (len(rows), NA, NG, BLK))


def by_blocks(x):
    e, c, w = x.shape
    return x.reshape(e, c, w // BLK, BLK).transpose(2, 1, 0, 3).reshape(w // BLK, c * e, BLK)


def local(
    positions,
    diffusion_noise,
    base_nuclei,
    displacements,
    charges,
    orbital_decay,
    coefficients,
    weights,
    counts,
    branch_source,
):
    blocks_here = counts.shape[0]
    peers = lax.axis_size(GX)
    replica = lax.axis_index("gz")
    member = lax.axis_index(GZY)
    device = lax.axis_index(GX)

    sent = by_blocks(positions)
    whole = lax.all_to_all(sent.reshape(EB, 2, 24, BLK), GZY, 0, 0, tiled=True)

    base = sent + STEP_ROOT * by_blocks(diffusion_noise)
    centers = base_nuclei[None, :, :] + displacements
    table = nucleus_table(centers, charges, orbital_decay, coefficients)
    nuclear = jnp.broadcast_to(nuclear_repulsion(centers, charges)[:, None], (NG, BLK))
    live = jnp.where(
        jnp.arange(BLK, dtype=jnp.int32)[None, :] < counts[:, None],
        weights.reshape(blocks_here, BLK),
        0.0,
    )
    own_live = lax.dynamic_slice_in_dim(live, member * 2, 2, 0)

    block_range = jnp.arange(blocks_here, dtype=jnp.int32)
    total = branch_source.shape[0]
    own_ids = device * blocks_here + block_range
    matches = (branch_source[None, :] == own_ids[:, None]).astype(jnp.int32)
    dest_slot = jnp.sum(matches * jnp.arange(total, dtype=jnp.int32)[None, :], axis=1)
    dest_device = dest_slot // blocks_here
    earlier = (
        (dest_device[None, :] == dest_device[:, None]) & (dest_slot[None, :] < dest_slot[:, None])
    ).astype(jnp.int32)
    send_slot = dest_device * CAP + jnp.sum(earlier, axis=1)
    selection = (
        jnp.arange(peers * CAP, dtype=jnp.int32)[:, None] == send_slot[None, :]
    ).astype(jnp.int32)
    picked = jnp.sum(selection * block_range[None, :], axis=1)
    my_sources = lax.dynamic_slice_in_dim(branch_source, device * blocks_here, blocks_here, 0)
    source_device = my_sources // blocks_here
    before = (
        (source_device[None, :] == source_device[:, None])
        & (block_range[None, :] < block_range[:, None])
    ).astype(jnp.int32)
    slots = source_device * CAP + jnp.sum(before, axis=1)

    out = walker_step(whole, table, nuclear, own_live)
    returned = lax.all_to_all(out, GZY, 0, 0, tiled=True).reshape(blocks_here, 32, BLK)
    send, local_energy = pack_step(picked, returned, base, live, peers)
    received = lax.all_to_all(send, GX, 0, 0, tiled=True)
    moved, new_weights, estimate = place_step(slots, replica.reshape(1), received)
    return (local_energy, estimate.reshape(NG // 2), moved, new_weights.reshape(blocks_here * BLK))


def solution(mesh):
    split = Mesh(
        mesh.devices.reshape(mesh.shape["gz"], 4, 4, mesh.shape["gy"]), ("gz", "gx_0", "gx_1", "gy")
    )
    placed = (
        P(("gz", "gy"), None, GX),
        P(("gz", "gy"), None, GX),
        P(),
        P(),
        P(),
        P(),
        P(),
        P(GX),
        P(GX),
        P(),
    )
    return jax.shard_map(
        local,
        mesh=split,
        in_specs=placed,
        out_specs=(P("gz", GX), P("gz"), P(("gz", "gy"), None, GX), P(GX)),
        check_vma=False,
    )
```

```python
import functools
import math

import jax
import jax.numpy as jnp
from jax import lax
from jax.experimental import pallas as pl
from jax.experimental.pallas import tpu as pltpu
from jax.sharding import Mesh
from jax.sharding import PartitionSpec as P

NE = 128
NA = 16
NG = 8
BLK = 128
EB = 16
CAP = 4
SLOT_ROWS = 24
PEER_ROWS = CAP * SLOT_ROWS + 8
GX = ("gx_0", "gx_1")
GZY = ("gz", "gy")

SOFT = 0.04
TIME_STEP = 0.01
STEP_ROOT = 0.1
LN2 = math.log(2.0)
LOG2E = 1.0 / LN2

K_CONST, K_X, K_Y, K_Z, K_R2, K_AMP, K_PHI, K_CX, K_CY, K_CZ, K_SOFT, K_POT = range(12)


def roll8(x, shift):
    shift %= 8
    return x if shift == 0 else pltpu.roll(x, shift, axis=0)


def pair_part(pos, rot, back, grad):
    zero = jnp.zeros((8, BLK), jnp.float32)

    def prepare(p, _):
        for h in range(2):
            for c in range(3):
                x = pos[p, h, c * 8 : c * 8 + 8, :]
                grad[p, h, c * 8 : c * 8 + 8, :] = zero
                for s in range(8):
                    rot[p, h, s, c * 8 : c * 8 + 8, :] = roll8(x, -s)
                    back[p, h, s, c * 8 : c * 8 + 8, :] = zero
        return 0

    lax.fori_loop(0, EB, prepare, 0)

    def terms(xi, xj, sums, half):
        d = [xi[c] - xj[c] for c in range(3)]
        square = (d[0] * d[0] + d[1] * d[1]) + (d[2] * d[2] + SOFT)
        inv = lax.rsqrt(square)
        p = 1.0 / (square * inv + 1.0)
        p2 = p * p
        slope = p2 * inv
        parts = (inv, slope, p2 * p, (inv * inv) * inv)
        if half:
            parts = tuple(0.5 * part for part in parts)
        return [slope * d[c] for c in range(3)], tuple(a + b for a, b in zip(sums, parts))

    def load3(ref, *at):
        return [ref[(*at, slice(c * 8, c * 8 + 8), slice(None))] for c in range(3)]

    def store3(ref, values, *at):
        for c in range(3):
            ref[(*at, slice(c * 8, c * 8 + 8), slice(None))] = values[c]

    def block_pair(i, j, h, xi, gi, sums):
        for s in range(8):
            f, sums = terms(xi, load3(rot, j, h, s), sums, False)
            gi = [gi[c] + f[c] for c in range(3)]
            b = load3(back, j, h, s)
            store3(back, [b[c] + f[c] for c in range(3)], j, h, s)
        return gi, sums

    def inside(t, sums):
        out = []
        for h in range(2):
            acc = sums[h]
            for i in (2 * t, 2 * t + 1):
                xi, gi = load3(pos, i, h), load3(grad, i, h)
                for s in range(1, 5):
                    f, acc = terms(xi, load3(rot, i, h, s), acc, s == 4)
                    gi = [gi[c] + f[c] for c in range(3)]
                    if s < 4:
                        b = load3(back, i, h, s)
                        store3(back, [b[c] + f[c] for c in range(3)], i, h, s)
                store3(grad, gi, i, h)
            i, j = 2 * t, 2 * t + 1
            gi, acc = block_pair(i, j, h, load3(pos, i, h), load3(grad, i, h), acc)
            store3(grad, gi, i, h)
            out.append(acc)
        return tuple(out)

    def across(u, t, sums):
        out = []
        for h in range(2):
            acc = sums[h]
            for i in (2 * u, 2 * u + 1):
                xi, gi = load3(pos, i, h), load3(grad, i, h)
                for j in (2 * t, 2 * t + 1):
                    gi, acc = block_pair(i, j, h, xi, gi, acc)
                store3(grad, gi, i, h)
            out.append(acc)
        return tuple(out)

    def outer(t, sums):
        sums = inside(t, sums)
        return lax.fori_loop(0, t, lambda u, carry: across(u, t, carry), sums)

    start = ((zero,) * 4, (zero,) * 4)
    sums = lax.fori_loop(0, EB // 2, outer, start)

    def finish(p, squares):
        out = []
        for h in range(2):
            acc = squares[h]
            for c in range(3):
                g = grad[p, h, c * 8 : c * 8 + 8, :]
                for s in range(8):
                    g = g - roll8(back[p, h, s, c * 8 : c * 8 + 8, :], s)
                g = 0.5 * g
                grad[p, h, c * 8 : c * 8 + 8, :] = g
                acc = acc + g * g
            out.append(acc)
        return tuple(out)

    squares = lax.fori_loop(0, EB, finish, (zero, zero))
    totals = []
    for h in range(2):
        inv, slope, cube, inv3 = sums[h]
        t = inv - (1.0 - 1.5 * SOFT) * slope + (1.0 - SOFT) * cube - (0.5 * SOFT) * inv3
        t = t - 0.5 * squares[h]
        totals.append(jnp.broadcast_to(jnp.sum(t, axis=0, keepdims=True), (8, BLK)))
    return totals


def walker_kernel(pos, table, nuclear, live, out, rot, back, grad):
    totals = pair_part(pos, rot, back, grad)
    zero = jnp.zeros((8, BLK), jnp.float32)

    def electrons(p, carry):
        energy, logs, pots = carry
        for e in range(8):
            xs, acc = [], []
            for h in range(2):
                x = [
                    jnp.broadcast_to(pos[p, h, c * 8 + e : c * 8 + e + 1, :], (8, BLK))
                    for c in range(3)
                ]
                xs.append((x[0], x[1], x[2], x[0] * x[0] + x[1] * x[1] + x[2] * x[2]))
                acc.append([zero] * 7)
            pots = list(pots)
            for a in range(NA):
                for h in range(2):
                    x, y, z, r2 = xs[h]
                    square = (r2 * table[K_R2, a] + table[K_CONST, a]) + (
                        (x * table[K_X, a] + y * table[K_Y, a]) + z * table[K_Z, a]
                    )
                    inv = lax.rsqrt(square)
                    amp = jnp.exp2(table[K_AMP, a] - square * inv)
                    u = amp * inv
                    s = acc[h]
                    acc[h] = [
                        s[0] + amp * table[K_PHI, a],
                        s[1] + amp,
                        s[2] + u,
                        s[3] + u * table[K_CX, a],
                        s[4] + u * table[K_CY, a],
                        s[5] + u * table[K_CZ, a],
                        s[6] + (u * inv) * ((inv + LN2) * table[K_SOFT, a]),
                    ]
                    pots[h] = pots[h] + inv * table[K_POT, a]
            new_energy, new_logs = [], []
            for h in range(2):
                phi, amps, us, ux, uy, uz, soft = acc[h]
                x, y, z, _ = xs[h]
                ratio = 1.0 / phi
                g = [(ux - x * us) * ratio, (uy - y * us) * ratio, (uz - z * us) * ratio]
                j = [
                    jnp.broadcast_to(grad[p, h, c * 8 + e : c * 8 + e + 1, :], (8, BLK))
                    for c in range(3)
                ]
                lap = (LN2 * amps - 2.0 * us - soft) * ratio
                dot = g[0] * j[0] + g[1] * j[1] + g[2] * j[2]
                new_energy.append(energy[h] - (0.5 * lap + dot))
                new_logs.append(logs[h] + jnp.log2(phi))
                for c in range(3):
                    out[p, h, c * 8 + e : c * 8 + e + 1, :] = (g[c] + j[c])[0:1, :]
            energy, logs = new_energy, new_logs
        return tuple(energy), tuple(logs), tuple(pots)

    energy, logs, pots = lax.fori_loop(
        0, EB, electrons, ((zero, zero), (zero, zero), (zero, zero))
    )
    row = lax.broadcasted_iota(jnp.int32, (8, BLK), 0)
    lane = lax.broadcasted_iota(jnp.int32, (8, BLK), 1)
    numerator = jnp.zeros((8, 1), jnp.float32)
    denominator = jnp.zeros((8, 1), jnp.float32)
    local = []
    for h in range(2):
        e = (energy[h] - pots[h] + totals[h] + nuclear[...]) * (1.0 / NE)
        weight = jnp.exp2(2.0 * (logs[h] - jnp.broadcast_to(logs[h][0:1, :], (8, BLK))))
        weight = weight * jnp.broadcast_to(live[h : h + 1, :], (8, BLK))
        numerator = numerator + jnp.sum(weight * e, axis=1, keepdims=True)
        denominator = denominator + jnp.sum(weight, axis=1, keepdims=True)
        local.append(e)
    placed = jnp.where(lane == row, numerator, 0.0) + jnp.where(lane == row + 8, denominator, 0.0)
    placed = jnp.broadcast_to(jnp.sum(placed, axis=0, keepdims=True), (8, BLK))
    for h in range(2):
        first = jnp.broadcast_to(local[h][0:1, :], (8, BLK))
        for half in range(2):
            e = local[h] if half == 0 else roll8(local[h], 4)
            tile = jnp.where(row < 4, e, jnp.where(row == 4, first, placed))
            for q in range(8):
                out[half * 8 + q, h, 24:32, :] = tile


def walker_step(whole, table, nuclear, live):
    vmem = pl.BlockSpec(memory_space=pltpu.VMEM)
    return pl.pallas_call(
        walker_kernel,
        out_shape=jax.ShapeDtypeStruct((EB, 2, 32, BLK), jnp.float32),
        in_specs=[vmem] * 4,
        out_specs=vmem,
        scratch_shapes=[
            pltpu.VMEM((EB, 2, 8, 24, BLK), jnp.float32),
            pltpu.VMEM((EB, 2, 8, 24, BLK), jnp.float32),
            pltpu.VMEM((EB, 2, 24, BLK), jnp.float32),
        ],
        compiler_params=pltpu.CompilerParams(vmem_limit_bytes=24 * 1024 * 1024),
        name="walker_step",
    )(whole, table, nuclear, live)


def pack_kernel(picked, returned, base, live, send, energy):
    sums = returned[0, 29:30, :]
    for p in range(1, EB):
        sums = sums + returned[2 * p, 29:30, :]
    for b in range(2 * EB):
        energy[:, b * BLK : (b + 1) * BLK] = returned[b, 24:28, :]

    def one_peer(peer, _):
        for k in range(CAP):
            b = picked[peer * CAP + k]
            for c in range(3):
                send[peer, k * 24 + c * 8 : k * 24 + c * 8 + 8, :] = (
                    base[b, c * 8 : c * 8 + 8, :] + TIME_STEP * returned[b, c * 8 : c * 8 + 8, :]
                )
            alive = live[pl.ds(b, 1), :]
            level = returned[b, 28:29, :] - jnp.log(alive)
            send[peer, 96 + k : 97 + k, :] = jnp.where(alive > 0.0, level, 3.0e38)
        send[peer, 100:101, :] = sums
        send[peer, 101:104, :] = jnp.zeros((3, BLK), jnp.float32)
        return 0

    lax.fori_loop(0, send.shape[0], one_peer, 0)


def pack_step(picked, returned, base, live, peers):
    vmem = pl.BlockSpec(memory_space=pltpu.VMEM)
    return pl.pallas_call(
        pack_kernel,
        out_shape=(
            jax.ShapeDtypeStruct((peers, PEER_ROWS, BLK), jnp.float32),
            jax.ShapeDtypeStruct((NG // 2, 2 * EB * BLK), jnp.float32),
        ),
        in_specs=[pl.BlockSpec(memory_space=pltpu.SMEM)] + [vmem] * 3,
        out_specs=(vmem, vmem),
        compiler_params=pltpu.CompilerParams(vmem_limit_bytes=8 * 1024 * 1024),
        name="pack_step",
    )(picked, returned, base, live)


def place_kernel(slots, half, received, moved, weights, estimate):
    sums = received[0, 100:101, :]
    for peer in range(1, received.shape[0]):
        sums = sums + received[peer, 100:101, :]
    sums = jnp.broadcast_to(sums, (8, BLK))
    ratio = sums / pltpu.roll(sums, BLK - 8, axis=1)
    lane = lax.broadcasted_iota(jnp.int32, (8, BLK), 1)
    reference = jnp.sum(jnp.where(lane == 0, ratio, 0.0), axis=1, keepdims=True)[0:1, :]
    own = jnp.where(half[0] == 0, ratio, pltpu.roll(ratio, BLK - 4, axis=1))
    estimate[...] = own[0:1, 0:4]
    for d in range(weights.shape[0]):
        peer, k = slots[d] // CAP, slots[d] % CAP
        for c in range(3):
            at = pl.multiple_of(k * 24 + c * 8, 8)
            moved[c, :, d * BLK : (d + 1) * BLK] = received[peer, pl.ds(at, 8), :]
        level = received[peer, pl.ds(96 + k, 1), :]
        weights[d : d + 1, :] = jnp.exp(-(level - reference))


def place_step(slots, half, received):
    vmem = pl.BlockSpec(memory_space=pltpu.VMEM)
    smem = pl.BlockSpec(memory_space=pltpu.SMEM)
    blocks = slots.shape[0]
    return pl.pallas_call(
        place_kernel,
        out_shape=(
            jax.ShapeDtypeStruct((3, 8, blocks * BLK), jnp.float32),
            jax.ShapeDtypeStruct((blocks, BLK), jnp.float32),
            jax.ShapeDtypeStruct((1, NG // 2), jnp.float32),
        ),
        in_specs=[smem, smem, vmem],
        out_specs=(vmem, vmem, vmem),
        compiler_params=pltpu.CompilerParams(vmem_limit_bytes=8 * 1024 * 1024),
        name="place_step",
    )(slots, half, received)


def nuclear_repulsion(centers, charges):
    offsets = centers[:, :, None, :] - centers[:, None, :, :]
    identity = jnp.eye(NA, dtype=jnp.float32)
    distance = jnp.sqrt(jnp.sum(offsets * offsets, axis=3) + identity)
    product = charges[:, None] * charges[None, :] * (1.0 - identity)
    return 0.5 * jnp.sum(product / distance, axis=(1, 2))


def nucleus_table(centers, charges, decay, coefficients):
    c = jnp.moveaxis(centers, 1, 0)
    k = (decay * LOG2E)[:, None]
    k2 = k * k
    scale = decay[:, None] * k
    ones = jnp.ones((NA, NG), jnp.float32)
    rows = [
        k2 * (jnp.sum(c * c, axis=2) + SOFT),
        -2.0 * k2 * c[:, :, 0],
        -2.0 * k2 * c[:, :, 1],
        -2.0 * k2 * c[:, :, 2],
        k2 * ones,
        jnp.log2(coefficients[:, None] * scale) * ones,
        ones / scale,
        c[:, :, 0],
        c[:, :, 1],
        c[:, :, 2],
        SOFT * k2 * ones,
        (charges[:, None] * k) * ones,
    ]
    return jnp.broadcast_to(jnp.stack(rows)[..., None], (len(rows), NA, NG, BLK))


def by_blocks(x):
    e, c, w = x.shape
    return x.reshape(e, c, w // BLK, BLK).transpose(2, 1, 0, 3).reshape(w // BLK, c * e, BLK)


def local(
    positions,
    diffusion_noise,
    base_nuclei,
    displacements,
    charges,
    orbital_decay,
    coefficients,
    weights,
    counts,
    branch_source,
):
    blocks_here = counts.shape[0]
    peers = lax.axis_size(GX)
    replica = lax.axis_index("gz")
    member = lax.axis_index(GZY)
    device = lax.axis_index(GX)

    sent = by_blocks(positions)
    whole = lax.all_to_all(sent.reshape(EB, 2, 24, BLK), GZY, 0, 0, tiled=True)

    base = sent + STEP_ROOT * by_blocks(diffusion_noise)
    centers = base_nuclei[None, :, :] + displacements
    table = nucleus_table(centers, charges, orbital_decay, coefficients)
    nuclear = jnp.broadcast_to(nuclear_repulsion(centers, charges)[:, None], (NG, BLK))
    live = jnp.where(
        jnp.arange(BLK, dtype=jnp.int32)[None, :] < counts[:, None],
        weights.reshape(blocks_here, BLK),
        0.0,
    )
    own_live = lax.dynamic_slice_in_dim(live, member * 2, 2, 0)

    block_range = jnp.arange(blocks_here, dtype=jnp.int32)
    total = branch_source.shape[0]
    own_ids = device * blocks_here + block_range
    matches = (branch_source[None, :] == own_ids[:, None]).astype(jnp.int32)
    dest_slot = jnp.sum(matches * jnp.arange(total, dtype=jnp.int32)[None, :], axis=1)
    dest_device = dest_slot // blocks_here
    earlier = (
        (dest_device[None, :] == dest_device[:, None]) & (dest_slot[None, :] < dest_slot[:, None])
    ).astype(jnp.int32)
    send_slot = dest_device * CAP + jnp.sum(earlier, axis=1)
    selection = (
        jnp.arange(peers * CAP, dtype=jnp.int32)[:, None] == send_slot[None, :]
    ).astype(jnp.int32)
    picked = jnp.sum(selection * block_range[None, :], axis=1)
    my_sources = lax.dynamic_slice_in_dim(branch_source, device * blocks_here, blocks_here, 0)
    source_device = my_sources // blocks_here
    before = (
        (source_device[None, :] == source_device[:, None])
        & (block_range[None, :] < block_range[:, None])
    ).astype(jnp.int32)
    slots = source_device * CAP + jnp.sum(before, axis=1)

    out = walker_step(whole, table, nuclear, own_live)
    returned = lax.all_to_all(out, GZY, 0, 0, tiled=True).reshape(blocks_here, 32, BLK)
    send, local_energy = pack_step(picked, returned, base, live, peers)
    received = lax.all_to_all(send, GX, 0, 0, tiled=True)
    moved, new_weights, estimate = place_step(slots, replica.reshape(1), received)
    return (local_energy, estimate.reshape(NG // 2), moved.transpose(1, 0, 2), new_weights.reshape(blocks_here * BLK))


def solution(mesh):
    split = Mesh(
        mesh.devices.reshape(mesh.shape["gz"], 4, 4, mesh.shape["gy"]), ("gz", "gx_0", "gx_1", "gy")
    )
    placed = (
        P(("gz", "gy"), None, GX),
        P(("gz", "gy"), None, GX),
        P(),
        P(),
        P(),
        P(),
        P(),
        P(GX),
        P(GX),
        P(),
    )
    return jax.shard_map(
        local,
        mesh=split,
        in_specs=placed,
        out_specs=(P("gz", GX), P("gz"), P(("gz", "gy"), None, GX), P(GX)),
        check_vma=False,
    )
```

```python
import functools
import math

import jax
import jax.numpy as jnp
from jax import lax
from jax.experimental import pallas as pl
from jax.experimental.pallas import tpu as pltpu
from jax.sharding import Mesh
from jax.sharding import PartitionSpec as P

NE = 128
NA = 16
NG = 8
BLK = 128
EB = 16
GROUP = 4
CAP = 4
SLOT_ROWS = 24
PEER_ROWS = CAP * SLOT_ROWS + 8
GX = ("gx_0", "gx_1")
GZY = ("gz", "gy")

SOFT = 0.04
TIME_STEP = 0.01
STEP_ROOT = 0.1
LN2 = math.log(2.0)
LOG2E = 1.0 / LN2

def roll8(x, shift):
    shift %= 8
    return x if shift == 0 else pltpu.roll(x, shift, axis=0)


def pair_part(pos, rot, back, grad):
    zero = jnp.zeros((8, BLK), jnp.float32)

    def prepare(p, _):
        for h in range(2):
            for c in range(3):
                x = pos[p, h, c * 8 : c * 8 + 8, :]
                grad[p, h, c * 8 : c * 8 + 8, :] = zero
                for s in range(8):
                    rot[p, h, s, c * 8 : c * 8 + 8, :] = roll8(x, -s)
                    back[p, h, s, c * 8 : c * 8 + 8, :] = zero
        return 0

    lax.fori_loop(0, EB, prepare, 0)

    def terms(xi, xj, sums, half):
        d = [xi[c] - xj[c] for c in range(3)]
        square = (d[0] * d[0] + d[1] * d[1]) + (d[2] * d[2] + SOFT)
        inv = lax.rsqrt(square)
        p = 1.0 / (square * inv + 1.0)
        p2 = p * p
        slope = p2 * inv
        parts = (inv, slope, p2 * p, (inv * inv) * inv)
        if half:
            parts = tuple(0.5 * part for part in parts)
        return [slope * d[c] for c in range(3)], tuple(a + b for a, b in zip(sums, parts))

    def load3(ref, *at):
        return [ref[(*at, slice(c * 8, c * 8 + 8), slice(None))] for c in range(3)]

    def store3(ref, values, *at):
        for c in range(3):
            ref[(*at, slice(c * 8, c * 8 + 8), slice(None))] = values[c]

    def block_pair(i, j, h, xi, gi, sums):
        for s in range(8):
            f, sums = terms(xi, load3(rot, j, h, s), sums, False)
            gi = [gi[c] + f[c] for c in range(3)]
            b = load3(back, j, h, s)
            store3(back, [b[c] + f[c] for c in range(3)], j, h, s)
        return gi, sums

    def inside(t, sums):
        out = []
        for h in range(2):
            acc = sums[h]
            for i in (2 * t, 2 * t + 1):
                xi, gi = load3(pos, i, h), load3(grad, i, h)
                for s in range(1, 5):
                    f, acc = terms(xi, load3(rot, i, h, s), acc, s == 4)
                    gi = [gi[c] + f[c] for c in range(3)]
                    if s < 4:
                        b = load3(back, i, h, s)
                        store3(back, [b[c] + f[c] for c in range(3)], i, h, s)
                store3(grad, gi, i, h)
            i, j = 2 * t, 2 * t + 1
            gi, acc = block_pair(i, j, h, load3(pos, i, h), load3(grad, i, h), acc)
            store3(grad, gi, i, h)
            out.append(acc)
        return tuple(out)

    def across(u, t, sums):
        out = []
        for h in range(2):
            acc = sums[h]
            for i in (2 * u, 2 * u + 1):
                xi, gi = load3(pos, i, h), load3(grad, i, h)
                for j in (2 * t, 2 * t + 1):
                    gi, acc = block_pair(i, j, h, xi, gi, acc)
                store3(grad, gi, i, h)
            out.append(acc)
        return tuple(out)

    def outer(t, sums):
        sums = inside(t, sums)
        return lax.fori_loop(0, t, lambda u, carry: across(u, t, carry), sums)

    start = ((zero,) * 4, (zero,) * 4)
    sums = lax.fori_loop(0, EB // 2, outer, start)

    def finish(p, squares):
        out = []
        for h in range(2):
            acc = squares[h]
            for c in range(3):
                g = grad[p, h, c * 8 : c * 8 + 8, :]
                for s in range(8):
                    g = g - roll8(back[p, h, s, c * 8 : c * 8 + 8, :], s)
                g = 0.5 * g
                grad[p, h, c * 8 : c * 8 + 8, :] = g
                acc = acc + g * g
            out.append(acc)
        return tuple(out)

    squares = lax.fori_loop(0, EB, finish, (zero, zero))
    totals = []
    for h in range(2):
        inv, slope, cube, inv3 = sums[h]
        t = inv - (1.0 - 1.5 * SOFT) * slope + (1.0 - SOFT) * cube - (0.5 * SOFT) * inv3
        t = t - 0.5 * squares[h]
        totals.append(jnp.broadcast_to(jnp.sum(t, axis=0, keepdims=True), (8, BLK)))
    return totals


def split3(x):
    high = x.astype(jnp.bfloat16).astype(jnp.float32)
    rest = x - high
    middle = rest.astype(jnp.bfloat16).astype(jnp.float32)
    return high, middle, rest - middle


def walker_kernel(
    pos, spread, sums, table, nuclear, live, out, rot, back, grad,
    left, right, square0, square1, parts0, parts1, held0, held1,
):
    totals = pair_part(pos, rot, back, grad)
    zero = jnp.zeros((8, BLK), jnp.float32)
    one = jnp.ones((8, BLK), jnp.float32)
    wide = jnp.zeros((16, BLK), jnp.float32)

    column = lax.broadcasted_iota(jnp.int32, (8 * NA, 2 * BLK), 1)
    for e in range(8):
        weights = jnp.where(column % 8 == e, spread[...], 0.0)
        left[e * 128 : e * 128 + 128, :] = weights
    for row in range(24, 32):
        right[row * 8 : row * 8 + 8, :] = jnp.full((8, 2 * BLK), 1.0 if row < 27 else 0.0)

    def features(p):
        for h in range(2):
            lanes = slice(h * BLK, h * BLK + BLK)
            x = [pos[p, h, c * 8 : c * 8 + 8, :] for c in range(3)]
            x.append(x[0] * x[0] + x[1] * x[1] + x[2] * x[2])
            tiles = []
            for value in x:
                high, middle, low = split3(value)
                tiles += [high, high, high, middle, middle, low]
            for row, tile in enumerate(tiles):
                right[row * 8 : row * 8 + 8, lanes] = tile

    def squares(square, first, count):
        rows = slice(first * 128, (first + count) * 128)
        square[rows, :] = jnp.dot(left[rows, :], right[...], preferred_element_type=jnp.float32)

    def orbitals(square, parts, held, pots, first, count):
        pots = list(pots)
        pair = jnp.zeros((16, BLK), jnp.float32)
        acc = {(e, h): [pair] * 2 for e in range(first, first + count) for h in range(2)}
        for a in range(0, NA * 8, 16):
            logs, phis, charge = (table[k, a : a + 16, :] for k in range(3))
            for h in range(2):
                lanes = slice(h * BLK, h * BLK + BLK)
                near = []
                for e in range(first, first + count):
                    sq = square[e * 128 + a : e * 128 + a + 16, lanes]
                    inv = lax.rsqrt(sq)
                    amp = jnp.exp2(logs - sq * inv)
                    u = amp * inv
                    s = acc[e, h]
                    acc[e, h] = [s[0] + amp * phis, s[1] + amp]
                    parts[e, 256 + a : 272 + a, lanes] = (u * inv) * (inv + LN2)
                    near.append(inv)
                    high = u.astype(jnp.bfloat16).astype(jnp.float32)
                    parts[e, a : a + 16, lanes] = high
                    parts[e, 128 + a : 144 + a, lanes] = u - high
                pots[h] = pots[h] + functools.reduce(jnp.add, near) * charge
        for (e, h), s in acc.items():
            for k in range(2):
                held[e, h, k] = s[k][0:8, :] + s[k][8:16, :]
        return tuple(pots)

    def gather(p, parts, held, energy, logs, first, count):
        energy, logs = list(energy), list(logs)
        for e in range(first, first + count):
            got = jnp.dot(sums[...], parts[e], preferred_element_type=jnp.float32)
            for h in range(2):
                lanes = slice(h * BLK, h * BLK + BLK)
                o = [got[k * 8 : k * 8 + 8, lanes] for k in range(9)]
                us, u = o[0], [o[1] + o[2], o[3] + o[4], o[5] + o[6]]
                phi, amps, soft = held[e, h, 0], held[e, h, 1], o[7] + o[8]
                ratio = 1.0 / phi
                at = [slice(c * 8 + e, c * 8 + e + 1) for c in range(3)]
                x = [jnp.broadcast_to(pos[p, h, at[c], :], (8, BLK)) for c in range(3)]
                j = [jnp.broadcast_to(grad[p, h, at[c], :], (8, BLK)) for c in range(3)]
                g = [(u[c] - x[c] * us) * ratio for c in range(3)]
                lap = (LN2 * amps - 2.0 * us - soft) * ratio
                dot = g[0] * j[0] + g[1] * j[1] + g[2] * j[2]
                energy[h] = energy[h] - (0.5 * lap + dot)
                logs[h] = logs[h] + jnp.log2(phi)
                for c in range(3):
                    out[p, h, at[c], :] = (g[c] + j[c])[0:1, :]
        return tuple(energy), tuple(logs)

    parts1[...] = jnp.zeros_like(parts1)
    for e in range(8):
        for h in range(2):
            held1[e, h, 0], held1[e, h, 1] = one, zero
    features(0)
    squares(square0, 0, 8)

    def one_block(p, now, later, parts, held, before, kept, carry):
        energy, logs, pots = carry
        features(jnp.minimum(p + 1, EB - 1))
        for first in range(0, 8, GROUP):
            squares(later, first, GROUP)
            pots = orbitals(now, parts, held, pots, first, GROUP)
            energy, logs = gather(jnp.maximum(p - 1, 0), before, kept, energy, logs, first, GROUP)
        return energy, logs, pots

    def two_blocks(t, carry):
        carry = one_block(2 * t, square0, square1, parts0, held0, parts1, held1, carry)
        return one_block(2 * t + 1, square1, square0, parts1, held1, parts0, held0, carry)

    energy, logs, pots = lax.fori_loop(
        0, EB // 2, two_blocks, ((zero, zero), (zero, zero), (wide, wide))
    )
    pots = [q[0:8, :] + q[8:16, :] for q in pots]
    energy, logs = gather(EB - 1, parts1, held1, energy, logs, 0, 8)
    row = lax.broadcasted_iota(jnp.int32, (8, BLK), 0)
    lane = lax.broadcasted_iota(jnp.int32, (8, BLK), 1)
    numerator = jnp.zeros((8, 1), jnp.float32)
    denominator = jnp.zeros((8, 1), jnp.float32)
    local = []
    for h in range(2):
        e = (energy[h] - pots[h] + totals[h] + nuclear[...]) * (1.0 / NE)
        weight = jnp.exp2(2.0 * (logs[h] - jnp.broadcast_to(logs[h][0:1, :], (8, BLK))))
        weight = weight * jnp.broadcast_to(live[h : h + 1, :], (8, BLK))
        numerator = numerator + jnp.sum(weight * e, axis=1, keepdims=True)
        denominator = denominator + jnp.sum(weight, axis=1, keepdims=True)
        local.append(e)
    placed = jnp.where(lane == row, numerator, 0.0) + jnp.where(lane == row + 8, denominator, 0.0)
    placed = jnp.broadcast_to(jnp.sum(placed, axis=0, keepdims=True), (8, BLK))
    for h in range(2):
        first = jnp.broadcast_to(local[h][0:1, :], (8, BLK))
        for half in range(2):
            e = local[h] if half == 0 else roll8(local[h], 4)
            tile = jnp.where(row < 4, e, jnp.where(row == 4, first, placed))
            for q in range(8):
                out[half * 8 + q, h, 24:32, :] = tile


def walker_step(whole, spread, sums, table, nuclear, live):
    vmem = pl.BlockSpec(memory_space=pltpu.VMEM)
    rows, width = 8 * NA * 8, 2 * BLK
    return pl.pallas_call(
        walker_kernel,
        out_shape=jax.ShapeDtypeStruct((EB, 2, 32, BLK), jnp.float32),
        in_specs=[vmem] * 6,
        out_specs=vmem,
        scratch_shapes=[
            pltpu.VMEM((EB, 2, 8, 24, BLK), jnp.float32),
            pltpu.VMEM((EB, 2, 8, 24, BLK), jnp.float32),
            pltpu.VMEM((EB, 2, 24, BLK), jnp.float32),
            pltpu.VMEM((rows, width), jnp.float32),
            pltpu.VMEM((width, width), jnp.float32),
            pltpu.VMEM((rows, width), jnp.float32),
            pltpu.VMEM((rows, width), jnp.float32),
            pltpu.VMEM((8, 3 * 8 * NA, width), jnp.float32),
            pltpu.VMEM((8, 3 * 8 * NA, width), jnp.float32),
            pltpu.VMEM((8, 2, 2, 8, BLK), jnp.float32),
            pltpu.VMEM((8, 2, 2, 8, BLK), jnp.float32),
        ],
        compiler_params=pltpu.CompilerParams(vmem_limit_bytes=24 * 1024 * 1024),
        name="walker_step",
    )(whole, spread, sums, table, nuclear, live)


def pack_kernel(picked, returned, base, live, send, energy):
    sums = returned[0, 29:30, :]
    for p in range(1, EB):
        sums = sums + returned[2 * p, 29:30, :]
    for b in range(2 * EB):
        energy[:, b * BLK : (b + 1) * BLK] = returned[b, 24:28, :]

    def one_peer(peer, _):
        for k in range(CAP):
            b = picked[peer * CAP + k]
            for c in range(3):
                send[peer, k * 24 + c * 8 : k * 24 + c * 8 + 8, :] = (
                    base[b, c * 8 : c * 8 + 8, :] + TIME_STEP * returned[b, c * 8 : c * 8 + 8, :]
                )
            alive = live[pl.ds(b, 1), :]
            level = returned[b, 28:29, :] - jnp.log(alive)
            send[peer, 96 + k : 97 + k, :] = jnp.where(alive > 0.0, level, 3.0e38)
        send[peer, 100:101, :] = sums
        send[peer, 101:104, :] = jnp.zeros((3, BLK), jnp.float32)
        return 0

    lax.fori_loop(0, send.shape[0], one_peer, 0)


def pack_step(picked, returned, base, live, peers):
    vmem = pl.BlockSpec(memory_space=pltpu.VMEM)
    return pl.pallas_call(
        pack_kernel,
        out_shape=(
            jax.ShapeDtypeStruct((peers, PEER_ROWS, BLK), jnp.float32),
            jax.ShapeDtypeStruct((NG // 2, 2 * EB * BLK), jnp.float32),
        ),
        in_specs=[pl.BlockSpec(memory_space=pltpu.SMEM)] + [vmem] * 3,
        out_specs=(vmem, vmem),
        compiler_params=pltpu.CompilerParams(vmem_limit_bytes=8 * 1024 * 1024),
        name="pack_step",
    )(picked, returned, base, live)


def place_kernel(slots, half, received, moved, weights, estimate):
    sums = received[0, 100:101, :]
    for peer in range(1, received.shape[0]):
        sums = sums + received[peer, 100:101, :]
    sums = jnp.broadcast_to(sums, (8, BLK))
    ratio = sums / pltpu.roll(sums, BLK - 8, axis=1)
    lane = lax.broadcasted_iota(jnp.int32, (8, BLK), 1)
    reference = jnp.sum(jnp.where(lane == 0, ratio, 0.0), axis=1, keepdims=True)[0:1, :]
    own = jnp.where(half[0] == 0, ratio, pltpu.roll(ratio, BLK - 4, axis=1))
    estimate[...] = own[0:1, 0:4]
    for d in range(weights.shape[0]):
        peer, k = slots[d] // CAP, slots[d] % CAP
        for c in range(3):
            at = pl.multiple_of(k * 24 + c * 8, 8)
            moved[c, :, d * BLK : (d + 1) * BLK] = received[peer, pl.ds(at, 8), :]
        level = received[peer, pl.ds(96 + k, 1), :]
        weights[d : d + 1, :] = jnp.exp(-(level - reference))


def place_step(slots, half, received):
    vmem = pl.BlockSpec(memory_space=pltpu.VMEM)
    smem = pl.BlockSpec(memory_space=pltpu.SMEM)
    blocks = slots.shape[0]
    return pl.pallas_call(
        place_kernel,
        out_shape=(
            jax.ShapeDtypeStruct((3, 8, blocks * BLK), jnp.float32),
            jax.ShapeDtypeStruct((blocks, BLK), jnp.float32),
            jax.ShapeDtypeStruct((1, NG // 2), jnp.float32),
        ),
        in_specs=[smem, smem, vmem],
        out_specs=(vmem, vmem, vmem),
        compiler_params=pltpu.CompilerParams(vmem_limit_bytes=8 * 1024 * 1024),
        name="place_step",
    )(slots, half, received)


def nuclear_repulsion(centers, charges):
    offsets = centers[:, :, None, :] - centers[:, None, :, :]
    identity = jnp.eye(NA, dtype=jnp.float32)
    distance = jnp.sqrt(jnp.sum(offsets * offsets, axis=3) + identity)
    product = charges[:, None] * charges[None, :] * (1.0 - identity)
    return 0.5 * jnp.sum(product / distance, axis=(1, 2))


def nucleus_tables(centers, charges, decay, coefficients):
    c = jnp.moveaxis(centers, 1, 0)
    k = (decay * LOG2E)[:, None]
    k2 = k * k
    scale = decay[:, None] * k
    ones = jnp.ones((NA, NG), jnp.float32)

    def thirds(x):
        high = lax.reduce_precision(x, 8, 7)
        rest = x - high
        middle = lax.reduce_precision(rest, 8, 7)
        return high, middle, rest - middle

    rows = []
    for value in [-2.0 * k2 * c[:, :, d] for d in range(3)] + [k2 * ones]:
        high, middle, low = thirds(value)
        rows += [high, middle, low, high, middle, high]
    rows += list(thirds(k2 * (jnp.sum(c * c, axis=2) + SOFT)))
    rows += [jnp.zeros_like(ones)] * (2 * BLK // 8 - len(rows))
    spread = jnp.stack(rows, axis=-1).reshape(NA * NG, len(rows), 1)
    spread = jnp.broadcast_to(spread, (NA * NG, len(rows), 8)).reshape(NA * NG, 2 * BLK)

    def halves(x):
        high = lax.reduce_precision(x, 8, 7)
        return [high, x - high]

    none = [0.0 * ones]
    weights = [ones] + sum((halves(c[:, :, d]) for d in range(3)), []) + 2 * none
    softs = 7 * none + halves(SOFT * k2 * ones)
    same = jnp.eye(NG, dtype=jnp.float32)

    def matrix(rows):
        full = jnp.stack(rows)[:, None, :, :] * same[None, :, None, :]
        return full.reshape(len(rows) * NG, NA * NG)

    sums = jnp.concatenate([matrix(weights), matrix(weights), matrix(softs)], axis=1)

    factors = [
        jnp.log2(coefficients * scale[:, 0]),
        1.0 / scale[:, 0],
        charges * k[:, 0],
    ]
    factors = jnp.stack(factors)[:, :, None, None]
    factors = jnp.broadcast_to(factors, (3, NA, NG, BLK)).reshape(3, NA * NG, BLK)
    return spread, sums, factors


def by_blocks(x):
    e, c, w = x.shape
    return x.reshape(e, c, w // BLK, BLK).transpose(2, 1, 0, 3).reshape(w // BLK, c * e, BLK)


def local(
    positions,
    diffusion_noise,
    base_nuclei,
    displacements,
    charges,
    orbital_decay,
    coefficients,
    weights,
    counts,
    branch_source,
):
    blocks_here = counts.shape[0]
    peers = lax.axis_size(GX)
    replica = lax.axis_index("gz")
    member = lax.axis_index(GZY)
    device = lax.axis_index(GX)

    sent = by_blocks(positions)
    whole = lax.all_to_all(sent.reshape(EB, 2, 24, BLK), GZY, 0, 0, tiled=True)

    base = sent + STEP_ROOT * by_blocks(diffusion_noise)
    centers = base_nuclei[None, :, :] + displacements
    spread, sums, table = nucleus_tables(centers, charges, orbital_decay, coefficients)
    nuclear = jnp.broadcast_to(nuclear_repulsion(centers, charges)[:, None], (NG, BLK))
    live = jnp.where(
        jnp.arange(BLK, dtype=jnp.int32)[None, :] < counts[:, None],
        weights.reshape(blocks_here, BLK),
        0.0,
    )
    own_live = lax.dynamic_slice_in_dim(live, member * 2, 2, 0)

    block_range = jnp.arange(blocks_here, dtype=jnp.int32)
    total = branch_source.shape[0]
    own_ids = device * blocks_here + block_range
    matches = (branch_source[None, :] == own_ids[:, None]).astype(jnp.int32)
    dest_slot = jnp.sum(matches * jnp.arange(total, dtype=jnp.int32)[None, :], axis=1)
    dest_device = dest_slot // blocks_here
    earlier = (
        (dest_device[None, :] == dest_device[:, None]) & (dest_slot[None, :] < dest_slot[:, None])
    ).astype(jnp.int32)
    send_slot = dest_device * CAP + jnp.sum(earlier, axis=1)
    selection = (
        jnp.arange(peers * CAP, dtype=jnp.int32)[:, None] == send_slot[None, :]
    ).astype(jnp.int32)
    picked = jnp.sum(selection * block_range[None, :], axis=1)
    my_sources = lax.dynamic_slice_in_dim(branch_source, device * blocks_here, blocks_here, 0)
    source_device = my_sources // blocks_here
    before = (
        (source_device[None, :] == source_device[:, None])
        & (block_range[None, :] < block_range[:, None])
    ).astype(jnp.int32)
    slots = source_device * CAP + jnp.sum(before, axis=1)

    out = walker_step(whole, spread, sums, table, nuclear, own_live)
    returned = lax.all_to_all(out, GZY, 0, 0, tiled=True).reshape(blocks_here, 32, BLK)
    send, local_energy = pack_step(picked, returned, base, live, peers)
    received = lax.all_to_all(send, GX, 0, 0, tiled=True)
    moved, new_weights, estimate = place_step(slots, replica.reshape(1), received)
    return (local_energy, estimate.reshape(NG // 2), moved.transpose(1, 0, 2), new_weights.reshape(blocks_here * BLK))


def solution(mesh):
    split = Mesh(
        mesh.devices.reshape(mesh.shape["gz"], 4, 4, mesh.shape["gy"]), ("gz", "gx_0", "gx_1", "gy")
    )
    placed = (
        P(("gz", "gy"), None, GX),
        P(("gz", "gy"), None, GX),
        P(),
        P(),
        P(),
        P(),
        P(),
        P(GX),
        P(GX),
        P(),
    )
    return jax.shard_map(
        local,
        mesh=split,
        in_specs=placed,
        out_specs=(P("gz", GX), P("gz"), P(("gz", "gy"), None, GX), P(GX)),
        check_vma=False,
    )
```

```python
import functools
import math

import jax
import jax.numpy as jnp
from jax import lax
from jax.experimental import pallas as pl
from jax.experimental.pallas import tpu as pltpu
from jax.sharding import Mesh
from jax.sharding import PartitionSpec as P

NE = 128
NA = 16
NG = 8
BLK = 128
EB = 16
GROUP = 4
CAP = 4
SLOT_ROWS = 24
PEER_ROWS = CAP * SLOT_ROWS + 8
GX = ("gx_0", "gx_1")
GZY = ("gz", "gy")

SOFT = 0.04
TIME_STEP = 0.01
STEP_ROOT = 0.1
LN2 = math.log(2.0)
LOG2E = 1.0 / LN2

def roll8(x, shift):
    shift %= 8
    return x if shift == 0 else pltpu.roll(x, shift, axis=0)


def pair_part(pos, rot, back, grad):
    zero = jnp.zeros((8, BLK), jnp.float32)

    def prepare(p, _):
        for h in range(2):
            for c in range(3):
                x = pos[p, h, c * 8 : c * 8 + 8, :]
                grad[p, h, c * 8 : c * 8 + 8, :] = zero
                for s in range(8):
                    rot[p, h, s, c * 8 : c * 8 + 8, :] = roll8(x, -s)
                    back[p, h, s, c * 8 : c * 8 + 8, :] = zero
        return 0

    lax.fori_loop(0, EB, prepare, 0)

    def terms(xi, xj, sums, half):
        d = [xi[c] - xj[c] for c in range(3)]
        square = (d[0] * d[0] + d[1] * d[1]) + (d[2] * d[2] + SOFT)
        inv = lax.rsqrt(square)
        p = 1.0 / (square * inv + 1.0)
        p2 = p * p
        slope = p2 * inv
        parts = (inv, slope, p2 * p, (inv * inv) * inv)
        if half:
            parts = tuple(0.5 * part for part in parts)
        return [slope * d[c] for c in range(3)], tuple(a + b for a, b in zip(sums, parts))

    def load3(ref, *at):
        return [ref[(*at, slice(c * 8, c * 8 + 8), slice(None))] for c in range(3)]

    def store3(ref, values, *at):
        for c in range(3):
            ref[(*at, slice(c * 8, c * 8 + 8), slice(None))] = values[c]

    def block_pair(i, j, h, xi, gi, sums):
        for s in range(8):
            f, sums = terms(xi, load3(rot, j, h, s), sums, False)
            gi = [gi[c] + f[c] for c in range(3)]
            b = load3(back, j, h, s)
            store3(back, [b[c] + f[c] for c in range(3)], j, h, s)
        return gi, sums

    def inside(t, sums):
        out = []
        for h in range(2):
            acc = sums[h]
            for i in (2 * t, 2 * t + 1):
                xi, gi = load3(pos, i, h), load3(grad, i, h)
                for s in range(1, 5):
                    f, acc = terms(xi, load3(rot, i, h, s), acc, s == 4)
                    gi = [gi[c] + f[c] for c in range(3)]
                    if s < 4:
                        b = load3(back, i, h, s)
                        store3(back, [b[c] + f[c] for c in range(3)], i, h, s)
                store3(grad, gi, i, h)
            i, j = 2 * t, 2 * t + 1
            gi, acc = block_pair(i, j, h, load3(pos, i, h), load3(grad, i, h), acc)
            store3(grad, gi, i, h)
            out.append(acc)
        return tuple(out)

    def across(u, t, sums):
        out = []
        for h in range(2):
            acc = sums[h]
            for i in (2 * u, 2 * u + 1):
                xi, gi = load3(pos, i, h), load3(grad, i, h)
                for j in (2 * t, 2 * t + 1):
                    gi, acc = block_pair(i, j, h, xi, gi, acc)
                store3(grad, gi, i, h)
            out.append(acc)
        return tuple(out)

    def outer(t, sums):
        sums = inside(t, sums)
        return lax.fori_loop(0, t, lambda u, carry: across(u, t, carry), sums)

    start = ((zero,) * 4, (zero,) * 4)
    sums = lax.fori_loop(0, EB // 2, outer, start)

    def finish(p, squares):
        out = []
        for h in range(2):
            acc = squares[h]
            for c in range(3):
                g = grad[p, h, c * 8 : c * 8 + 8, :]
                for s in range(8):
                    g = g - roll8(back[p, h, s, c * 8 : c * 8 + 8, :], s)
                g = 0.5 * g
                grad[p, h, c * 8 : c * 8 + 8, :] = g
                acc = acc + g * g
            out.append(acc)
        return tuple(out)

    squares = lax.fori_loop(0, EB, finish, (zero, zero))
    totals = []
    for h in range(2):
        inv, slope, cube, inv3 = sums[h]
        t = inv - (1.0 - 1.5 * SOFT) * slope + (1.0 - SOFT) * cube - (0.5 * SOFT) * inv3
        t = t - 0.5 * squares[h]
        totals.append(jnp.broadcast_to(jnp.sum(t, axis=0, keepdims=True), (8, BLK)))
    return totals


def split3(x):
    high = x.astype(jnp.bfloat16).astype(jnp.float32)
    rest = x - high
    middle = rest.astype(jnp.bfloat16).astype(jnp.float32)
    return high, middle, rest - middle


def pair_kernel(pos, grad, totals, rot, back):
    for h, total in enumerate(pair_part(pos, rot, back, grad)):
        totals[h] = total


def orbital_kernel(
    pos, grad, totals, spread, sums, table, nuclear, live, out,
    left, right, square0, square1, parts0, parts1, held0, held1,
):
    zero = jnp.zeros((8, BLK), jnp.float32)
    one = jnp.ones((8, BLK), jnp.float32)
    wide = jnp.zeros((16, BLK), jnp.float32)

    column = lax.broadcasted_iota(jnp.int32, (8 * NA, 2 * BLK), 1)
    for e in range(8):
        weights = jnp.where(column % 8 == e, spread[...], 0.0)
        left[e * 128 : e * 128 + 128, :] = weights.astype(jnp.bfloat16)
    for row in range(24, 32):
        right[row * 8 : row * 8 + 8, :] = jnp.full((8, 2 * BLK), 1.0 if row < 27 else 0.0)

    def features(p):
        for h in range(2):
            lanes = slice(h * BLK, h * BLK + BLK)
            x = [pos[p, h, c * 8 : c * 8 + 8, :] for c in range(3)]
            x.append(x[0] * x[0] + x[1] * x[1] + x[2] * x[2])
            tiles = []
            for value in x:
                high, middle, low = split3(value)
                tiles += [high, high, high, middle, middle, low]
            for row, tile in enumerate(tiles):
                right[row * 8 : row * 8 + 8, lanes] = tile

    def squares(square, first, count):
        rows = slice(first * 128, (first + count) * 128)
        factor = right[...].astype(jnp.bfloat16)
        square[rows, :] = jnp.dot(left[rows, :], factor, preferred_element_type=jnp.float32)

    def orbitals(square, parts, held, pots, first, count):
        pots = list(pots)
        pair = jnp.zeros((16, BLK), jnp.float32)
        acc = {(e, h): [pair] * 2 for e in range(first, first + count) for h in range(2)}
        for a in range(0, NA * 8, 16):
            logs, phis, charge = (table[k, a : a + 16, :] for k in range(3))
            for h in range(2):
                lanes = slice(h * BLK, h * BLK + BLK)
                near = []
                for e in range(first, first + count):
                    sq = square[e * 128 + a : e * 128 + a + 16, lanes]
                    inv = lax.rsqrt(sq)
                    amp = jnp.exp2(logs - sq * inv)
                    u = amp * inv
                    s = acc[e, h]
                    acc[e, h] = [s[0] + amp * phis, s[1] + amp]
                    parts[e, 256 + a : 272 + a, lanes] = (u * inv) * (inv + LN2)
                    near.append(inv)
                    high = u.astype(jnp.bfloat16).astype(jnp.float32)
                    parts[e, a : a + 16, lanes] = high
                    parts[e, 128 + a : 144 + a, lanes] = u - high
                pots[h] = pots[h] + functools.reduce(jnp.add, near) * charge
        for (e, h), s in acc.items():
            for k in range(2):
                held[e, h, k] = s[k][0:8, :] + s[k][8:16, :]
        return tuple(pots)

    def gather(p, parts, held, energy, logs, first, count):
        energy, logs = list(energy), list(logs)
        for e in range(first, first + count):
            factor = parts[e].astype(jnp.bfloat16)
            got = jnp.dot(sums[...], factor, preferred_element_type=jnp.float32)
            for h in range(2):
                lanes = slice(h * BLK, h * BLK + BLK)
                o = [got[k * 8 : k * 8 + 8, lanes] for k in range(9)]
                us, u = o[0], [o[1] + o[2], o[3] + o[4], o[5] + o[6]]
                phi, amps, soft = held[e, h, 0], held[e, h, 1], o[7] + o[8]
                ratio = 1.0 / phi
                at = [slice(c * 8 + e, c * 8 + e + 1) for c in range(3)]
                x = [jnp.broadcast_to(pos[p, h, at[c], :], (8, BLK)) for c in range(3)]
                j = [jnp.broadcast_to(grad[p, h, at[c], :], (8, BLK)) for c in range(3)]
                g = [(u[c] - x[c] * us) * ratio for c in range(3)]
                lap = (LN2 * amps - 2.0 * us - soft) * ratio
                dot = g[0] * j[0] + g[1] * j[1] + g[2] * j[2]
                energy[h] = energy[h] - (0.5 * lap + dot)
                logs[h] = logs[h] + jnp.log2(phi)
        return tuple(energy), tuple(logs)

    parts1[...] = jnp.zeros_like(parts1)
    for e in range(8):
        for h in range(2):
            held1[e, h, 0], held1[e, h, 1] = one, zero
    features(0)
    squares(square0, 0, 8)

    def one_block(p, now, later, parts, held, before, kept, carry):
        energy, logs, pots = carry
        features(jnp.minimum(p + 1, EB - 1))
        for first in range(0, 8, GROUP):
            squares(later, first, GROUP)
            pots = orbitals(now, parts, held, pots, first, GROUP)
            energy, logs = gather(jnp.maximum(p - 1, 0), before, kept, energy, logs, first, GROUP)
        return energy, logs, pots

    def two_blocks(t, carry):
        carry = one_block(2 * t, square0, square1, parts0, held0, parts1, held1, carry)
        return one_block(2 * t + 1, square1, square0, parts1, held1, parts0, held0, carry)

    energy, logs, pots = lax.fori_loop(
        0, EB // 2, two_blocks, ((zero, zero), (zero, zero), (wide, wide))
    )
    pots = [q[0:8, :] + q[8:16, :] for q in pots]
    energy, logs = gather(EB - 1, parts1, held1, energy, logs, 0, 8)
    row = lax.broadcasted_iota(jnp.int32, (8, BLK), 0)
    lane = lax.broadcasted_iota(jnp.int32, (8, BLK), 1)
    numerator = jnp.zeros((8, 1), jnp.float32)
    denominator = jnp.zeros((8, 1), jnp.float32)
    local = []
    for h in range(2):
        e = (energy[h] - pots[h] + totals[h] + nuclear[...]) * (1.0 / NE)
        weight = jnp.exp2(2.0 * (logs[h] - jnp.broadcast_to(logs[h][0:1, :], (8, BLK))))
        weight = weight * jnp.broadcast_to(live[h : h + 1, :], (8, BLK))
        numerator = numerator + jnp.sum(weight * e, axis=1, keepdims=True)
        denominator = denominator + jnp.sum(weight, axis=1, keepdims=True)
        local.append(e)
    placed = jnp.where(lane == row, numerator, 0.0) + jnp.where(lane == row + 8, denominator, 0.0)
    placed = jnp.broadcast_to(jnp.sum(placed, axis=0, keepdims=True), (8, BLK))
    firsts = [jnp.broadcast_to(local[h][0:1, :], (8, BLK)) for h in range(2)]
    rest = jnp.where(row == 0, firsts[0], jnp.where(row == 1, firsts[1], placed))
    for q in range(EB):
        low, high = local if q < EB // 2 else (roll8(local[0], 4), roll8(local[1], 4))
        out[q, 0:8, :] = jnp.where(row < 4, low, roll8(high, 4))
        out[q, 8:16, :] = rest


def pair_step(whole):
    vmem = pl.BlockSpec(memory_space=pltpu.VMEM)
    return pl.pallas_call(
        pair_kernel,
        out_shape=(
            jax.ShapeDtypeStruct((EB, 2, 24, BLK), jnp.float32),
            jax.ShapeDtypeStruct((2, 8, BLK), jnp.float32),
        ),
        in_specs=[vmem],
        out_specs=(vmem, vmem),
        scratch_shapes=[pltpu.VMEM((EB, 2, 8, 24, BLK), jnp.float32)] * 2,
        compiler_params=pltpu.CompilerParams(vmem_limit_bytes=16 * 1024 * 1024),
        cost_estimate=pl.CostEstimate(
            flops=EB * EB * BLK * 2 * 32 * 32, transcendentals=0, bytes_accessed=1 << 20
        ),
        name="pair_step",
    )(whole)


def orbital_step(whole, grad, totals, spread, sums, table, nuclear, live):
    vmem = pl.BlockSpec(memory_space=pltpu.VMEM)
    rows, width = 8 * NA * 8, 2 * BLK
    return pl.pallas_call(
        orbital_kernel,
        out_shape=jax.ShapeDtypeStruct((EB, 16, BLK), jnp.float32),
        in_specs=[vmem] * 8,
        out_specs=vmem,
        scratch_shapes=[
            pltpu.VMEM((rows, width), jnp.bfloat16),
            pltpu.VMEM((width, width), jnp.float32),
            pltpu.VMEM((rows, width), jnp.float32),
            pltpu.VMEM((rows, width), jnp.float32),
            pltpu.VMEM((8, 3 * 8 * NA, width), jnp.float32),
            pltpu.VMEM((8, 3 * 8 * NA, width), jnp.float32),
            pltpu.VMEM((8, 2, 2, 8, BLK), jnp.float32),
            pltpu.VMEM((8, 2, 2, 8, BLK), jnp.float32),
        ],
        compiler_params=pltpu.CompilerParams(vmem_limit_bytes=20 * 1024 * 1024),
        cost_estimate=pl.CostEstimate(
            flops=EB * 8 * NA * NG * BLK * 2 * 32 * 2, transcendentals=0, bytes_accessed=1 << 20
        ),
        name="orbital_step",
    )(whole, grad, totals, spread, sums, table, nuclear, live)


def own_kernel(scalars, positions, noise, base):
    wide = 4 * BLK

    def four(t, _):
        at = pl.multiple_of(t * wide, wide)
        r = [positions[c, :, pl.ds(at, wide)] for c in range(3)]
        phi = jnp.zeros((8, wide), jnp.float32)
        grad = [phi, phi, phi]
        for a in range(NA):
            v = [r[c] - scalars[c, a] for c in range(3)]
            square = (v[0] * v[0] + v[1] * v[1]) + (v[2] * v[2] + SOFT)
            inv = lax.rsqrt(square)
            amp = jnp.exp2(scalars[4, a] - scalars[3, a] * (square * inv))
            u = amp * inv
            phi = phi + amp * scalars[5, a]
            grad = [grad[c] + u * v[c] for c in range(3)]
        step = TIME_STEP / phi
        for c in range(3):
            moved = r[c] + STEP_ROOT * noise[c, :, pl.ds(at, wide)] - step * grad[c]
            for k in range(4):
                base[t * 4 + k, c * 8 : c * 8 + 8, :] = moved[:, k * BLK : (k + 1) * BLK]
        return 0

    lax.fori_loop(0, base.shape[0] // 4, four, 0)


def own_step(scalars, positions, noise):
    vmem = pl.BlockSpec(memory_space=pltpu.VMEM)
    blocks = positions.shape[2] // BLK
    return pl.pallas_call(
        own_kernel,
        out_shape=jax.ShapeDtypeStruct((blocks, 24, BLK), jnp.float32),
        in_specs=[pl.BlockSpec(memory_space=pltpu.SMEM), vmem, vmem],
        out_specs=vmem,
        compiler_params=pltpu.CompilerParams(vmem_limit_bytes=8 * 1024 * 1024),
        name="own_step",
    )(scalars, positions, noise)


def pack_kernel(picked, returned, energies, base, live, send, energy):
    sums = energies[0, 10:11, :]
    for p in range(1, EB):
        sums = sums + energies[p, 10:11, :]
    for b in range(2 * EB):
        at = (b % 2) * 4
        energy[:, b * BLK : (b + 1) * BLK] = energies[b // 2, at : at + 4, :]

    def one_peer(peer, _):
        for k in range(CAP):
            b = picked[peer * CAP + k]
            for c in range(3):
                send[peer, k * 24 + c * 8 : k * 24 + c * 8 + 8, :] = (
                    base[b, c * 8 : c * 8 + 8, :] + TIME_STEP * returned[b, c * 8 : c * 8 + 8, :]
                )
            alive = live[pl.ds(b, 1), :]
            level = energies[b // 2, pl.ds(8 + b % 2, 1), :] - jnp.log(alive)
            send[peer, 96 + k : 97 + k, :] = jnp.where(alive > 0.0, level, 3.0e38)
        send[peer, 100:101, :] = sums
        send[peer, 101:104, :] = jnp.zeros((3, BLK), jnp.float32)
        return 0

    lax.fori_loop(0, send.shape[0], one_peer, 0)


def pack_step(picked, returned, energies, base, live, peers):
    vmem = pl.BlockSpec(memory_space=pltpu.VMEM)
    return pl.pallas_call(
        pack_kernel,
        out_shape=(
            jax.ShapeDtypeStruct((peers, PEER_ROWS, BLK), jnp.float32),
            jax.ShapeDtypeStruct((NG // 2, 2 * EB * BLK), jnp.float32),
        ),
        in_specs=[pl.BlockSpec(memory_space=pltpu.SMEM)] + [vmem] * 4,
        out_specs=(vmem, vmem),
        compiler_params=pltpu.CompilerParams(vmem_limit_bytes=8 * 1024 * 1024),
        name="pack_step",
    )(picked, returned, energies, base, live)


def place_kernel(slots, half, received, moved, weights, estimate):
    sums = received[0, 100:101, :]
    for peer in range(1, received.shape[0]):
        sums = sums + received[peer, 100:101, :]
    sums = jnp.broadcast_to(sums, (8, BLK))
    ratio = sums / pltpu.roll(sums, BLK - 8, axis=1)
    lane = lax.broadcasted_iota(jnp.int32, (8, BLK), 1)
    reference = jnp.sum(jnp.where(lane == 0, ratio, 0.0), axis=1, keepdims=True)[0:1, :]
    own = jnp.where(half[0] == 0, ratio, pltpu.roll(ratio, BLK - 4, axis=1))
    estimate[...] = own[0:1, 0:4]
    for d in range(weights.shape[0]):
        peer, k = slots[d] // CAP, slots[d] % CAP
        for c in range(3):
            at = pl.multiple_of(k * 24 + c * 8, 8)
            moved[c, :, d * BLK : (d + 1) * BLK] = received[peer, pl.ds(at, 8), :]
        level = received[peer, pl.ds(96 + k, 1), :]
        weights[d : d + 1, :] = jnp.exp(-(level - reference))


def place_step(slots, half, received):
    vmem = pl.BlockSpec(memory_space=pltpu.VMEM)
    smem = pl.BlockSpec(memory_space=pltpu.SMEM)
    blocks = slots.shape[0]
    return pl.pallas_call(
        place_kernel,
        out_shape=(
            jax.ShapeDtypeStruct((3, 8, blocks * BLK), jnp.float32),
            jax.ShapeDtypeStruct((blocks, BLK), jnp.float32),
            jax.ShapeDtypeStruct((1, NG // 2), jnp.float32),
        ),
        in_specs=[smem, smem, vmem],
        out_specs=(vmem, vmem, vmem),
        compiler_params=pltpu.CompilerParams(vmem_limit_bytes=8 * 1024 * 1024),
        name="place_step",
    )(slots, half, received)


def nuclear_repulsion(centers, charges):
    offsets = centers[:, :, None, :] - centers[:, None, :, :]
    identity = jnp.eye(NA, dtype=jnp.float32)
    distance = jnp.sqrt(jnp.sum(offsets * offsets, axis=3) + identity)
    product = charges[:, None] * charges[None, :] * (1.0 - identity)
    return 0.5 * jnp.sum(product / distance, axis=(1, 2))


def nucleus_tables(centers, charges, decay, coefficients):
    c = jnp.moveaxis(centers, 1, 0)
    k = (decay * LOG2E)[:, None]
    k2 = k * k
    scale = decay[:, None] * k
    ones = jnp.ones((NA, NG), jnp.float32)

    def thirds(x):
        high = lax.reduce_precision(x, 8, 7)
        rest = x - high
        middle = lax.reduce_precision(rest, 8, 7)
        return high, middle, rest - middle

    rows = []
    for value in [-2.0 * k2 * c[:, :, d] for d in range(3)] + [k2 * ones]:
        high, middle, low = thirds(value)
        rows += [high, middle, low, high, middle, high]
    rows += list(thirds(k2 * (jnp.sum(c * c, axis=2) + SOFT)))
    rows += [jnp.zeros_like(ones)] * (2 * BLK // 8 - len(rows))
    spread = jnp.stack(rows, axis=-1).reshape(NA * NG, len(rows), 1)
    spread = jnp.broadcast_to(spread, (NA * NG, len(rows), 8)).reshape(NA * NG, 2 * BLK)

    def halves(x):
        high = lax.reduce_precision(x, 8, 7)
        return [high, x - high]

    none = [0.0 * ones]
    weights = [ones] + sum((halves(c[:, :, d]) for d in range(3)), []) + 2 * none
    softs = 7 * none + halves(SOFT * k2 * ones)
    same = jnp.eye(NG, dtype=jnp.float32)

    def matrix(rows):
        full = jnp.stack(rows)[:, None, :, :] * same[None, :, None, :]
        return full.reshape(len(rows) * NG, NA * NG)

    sums = jnp.concatenate([matrix(weights), matrix(weights), matrix(softs)], axis=1)
    sums = sums.astype(jnp.bfloat16)

    factors = [
        jnp.log2(coefficients * scale[:, 0]),
        1.0 / scale[:, 0],
        charges * k[:, 0],
    ]
    factors = jnp.stack(factors)[:, :, None, None]
    factors = jnp.broadcast_to(factors, (3, NA, NG, BLK)).reshape(3, NA * NG, BLK)
    return spread, sums, factors


def by_blocks(x):
    e, c, w = x.shape
    return x.reshape(e, c, w // BLK, BLK).transpose(2, 1, 0, 3).reshape(w // BLK, c * e, BLK)


def local(
    positions,
    diffusion_noise,
    base_nuclei,
    displacements,
    charges,
    orbital_decay,
    coefficients,
    weights,
    counts,
    branch_source,
):
    blocks_here = counts.shape[0]
    peers = lax.axis_size(GX)
    replica = lax.axis_index("gz")
    member = lax.axis_index(GZY)
    device = lax.axis_index(GX)

    sent = by_blocks(positions)
    whole = lax.all_to_all(sent.reshape(EB, 2, 24, BLK), GZY, 0, 0, tiled=True)

    centers = base_nuclei[None, :, :] + displacements
    first = centers[0]
    rate = orbital_decay * LOG2E
    level = jnp.log2(coefficients * orbital_decay)
    scalars = jnp.stack([first[:, 0], first[:, 1], first[:, 2], rate, level, 1.0 / orbital_decay])
    base = own_step(scalars, positions.transpose(1, 0, 2), diffusion_noise.transpose(1, 0, 2))
    spread, sums, table = nucleus_tables(centers, charges, orbital_decay, coefficients)
    nuclear = jnp.broadcast_to(nuclear_repulsion(centers, charges)[:, None], (NG, BLK))
    live = jnp.where(
        jnp.arange(BLK, dtype=jnp.int32)[None, :] < counts[:, None],
        weights.reshape(blocks_here, BLK),
        0.0,
    )
    own_live = lax.dynamic_slice_in_dim(live, member * 2, 2, 0)

    block_range = jnp.arange(blocks_here, dtype=jnp.int32)
    total = branch_source.shape[0]
    own_ids = device * blocks_here + block_range
    matches = (branch_source[None, :] == own_ids[:, None]).astype(jnp.int32)
    dest_slot = jnp.sum(matches * jnp.arange(total, dtype=jnp.int32)[None, :], axis=1)
    dest_device = dest_slot // blocks_here
    earlier = (
        (dest_device[None, :] == dest_device[:, None]) & (dest_slot[None, :] < dest_slot[:, None])
    ).astype(jnp.int32)
    send_slot = dest_device * CAP + jnp.sum(earlier, axis=1)
    selection = (
        jnp.arange(peers * CAP, dtype=jnp.int32)[:, None] == send_slot[None, :]
    ).astype(jnp.int32)
    picked = jnp.sum(selection * block_range[None, :], axis=1)
    my_sources = lax.dynamic_slice_in_dim(branch_source, device * blocks_here, blocks_here, 0)
    source_device = my_sources // blocks_here
    before = (
        (source_device[None, :] == source_device[:, None])
        & (block_range[None, :] < block_range[:, None])
    ).astype(jnp.int32)
    slots = source_device * CAP + jnp.sum(before, axis=1)

    whole, base, spread, sums, table, nuclear, own_live, picked = lax.optimization_barrier(
        (whole, base, spread, sums, table, nuclear, own_live, picked)
    )
    grad, totals = pair_step(whole)
    returned = lax.all_to_all(grad, GZY, 0, 0, tiled=True).reshape(blocks_here, 24, BLK)
    out = orbital_step(whole, grad, totals, spread, sums, table, nuclear, own_live)
    returned, out = lax.optimization_barrier((returned, out))
    energies = lax.all_to_all(out, GZY, 0, 0, tiled=True)
    send, local_energy = pack_step(picked, returned, energies, base, live, peers)
    received = lax.all_to_all(send, GX, 0, 0, tiled=True)
    moved, new_weights, estimate = place_step(slots, replica.reshape(1), received)
    return (local_energy, estimate.reshape(NG // 2), moved.transpose(1, 0, 2), new_weights.reshape(blocks_here * BLK))


def solution(mesh):
    split = Mesh(
        mesh.devices.reshape(mesh.shape["gz"], 4, 4, mesh.shape["gy"]), ("gz", "gx_0", "gx_1", "gy")
    )
    placed = (
        P(("gz", "gy"), None, GX),
        P(("gz", "gy"), None, GX),
        P(),
        P(),
        P(),
        P(),
        P(),
        P(GX),
        P(GX),
        P(),
    )
    return jax.shard_map(
        local,
        mesh=split,
        in_specs=placed,
        out_specs=(P("gz", GX), P("gz"), P(("gz", "gy"), None, GX), P(GX)),
        check_vma=False,
    )
```

```python
import functools
import math

import jax
import jax.numpy as jnp
from jax import lax
from jax.experimental import pallas as pl
from jax.experimental.pallas import tpu as pltpu
from jax.sharding import Mesh
from jax.sharding import PartitionSpec as P

NE = 128
NA = 16
NG = 8
BLK = 128
EB = 16
GROUP = 4
CAP = 4
SLOT_ROWS = 24
PEER_ROWS = CAP * SLOT_ROWS + 8
GX = ("gx_0", "gx_1")
GZY = ("gz", "gy")

SOFT = 0.04
TIME_STEP = 0.01
STEP_ROOT = 0.1
LN2 = math.log(2.0)
LOG2E = 1.0 / LN2

def roll8(x, shift):
    shift %= 8
    return x if shift == 0 else pltpu.roll(x, shift, axis=0)


def pair_part(pos, rot, back, grad):
    zero = jnp.zeros((8, BLK), jnp.float32)

    def prepare(p, _):
        for h in range(2):
            for c in range(3):
                x = pos[p, h, c * 8 : c * 8 + 8, :]
                grad[p, h, c * 8 : c * 8 + 8, :] = zero
                for s in range(8):
                    rot[p, h, s, c * 8 : c * 8 + 8, :] = roll8(x, -s)
                    back[p, h, s, c * 8 : c * 8 + 8, :] = zero
        return 0

    lax.fori_loop(0, EB, prepare, 0)

    def terms(xi, xj, sums, half):
        d = [xi[c] - xj[c] for c in range(3)]
        square = (d[0] * d[0] + d[1] * d[1]) + (d[2] * d[2] + SOFT)
        inv = lax.rsqrt(square)
        p = 1.0 / (square * inv + 1.0)
        p2 = p * p
        slope = p2 * inv
        parts = (inv, slope, p2 * p, (inv * inv) * inv)
        if half:
            parts = tuple(0.5 * part for part in parts)
        return [slope * d[c] for c in range(3)], tuple(a + b for a, b in zip(sums, parts))

    def load3(ref, *at):
        return [ref[(*at, slice(c * 8, c * 8 + 8), slice(None))] for c in range(3)]

    def store3(ref, values, *at):
        for c in range(3):
            ref[(*at, slice(c * 8, c * 8 + 8), slice(None))] = values[c]

    def block_pair(i, j, h, xi, gi, sums):
        for s in range(8):
            f, sums = terms(xi, load3(rot, j, h, s), sums, False)
            gi = [gi[c] + f[c] for c in range(3)]
            b = load3(back, j, h, s)
            store3(back, [b[c] + f[c] for c in range(3)], j, h, s)
        return gi, sums

    def inside(t, sums):
        out = []
        for h in range(2):
            acc = sums[h]
            for i in (2 * t, 2 * t + 1):
                xi, gi = load3(pos, i, h), load3(grad, i, h)
                for s in range(1, 5):
                    f, acc = terms(xi, load3(rot, i, h, s), acc, s == 4)
                    gi = [gi[c] + f[c] for c in range(3)]
                    if s < 4:
                        b = load3(back, i, h, s)
                        store3(back, [b[c] + f[c] for c in range(3)], i, h, s)
                store3(grad, gi, i, h)
            i, j = 2 * t, 2 * t + 1
            gi, acc = block_pair(i, j, h, load3(pos, i, h), load3(grad, i, h), acc)
            store3(grad, gi, i, h)
            out.append(acc)
        return tuple(out)

    def across(u, t, sums):
        out = []
        for h in range(2):
            acc = sums[h]
            for i in (2 * u, 2 * u + 1):
                xi, gi = load3(pos, i, h), load3(grad, i, h)
                for j in (2 * t, 2 * t + 1):
                    gi, acc = block_pair(i, j, h, xi, gi, acc)
                store3(grad, gi, i, h)
            out.append(acc)
        return tuple(out)

    def outer(t, sums):
        sums = inside(t, sums)
        return lax.fori_loop(0, t, lambda u, carry: across(u, t, carry), sums)

    start = ((zero,) * 4, (zero,) * 4)
    sums = lax.fori_loop(0, EB // 2, outer, start)

    def finish(p, squares):
        out = []
        for h in range(2):
            acc = squares[h]
            for c in range(3):
                g = grad[p, h, c * 8 : c * 8 + 8, :]
                for s in range(8):
                    g = g - roll8(back[p, h, s, c * 8 : c * 8 + 8, :], s)
                g = 0.5 * g
                grad[p, h, c * 8 : c * 8 + 8, :] = g
                acc = acc + g * g
            out.append(acc)
        return tuple(out)

    squares = lax.fori_loop(0, EB, finish, (zero, zero))
    totals = []
    for h in range(2):
        inv, slope, cube, inv3 = sums[h]
        t = inv - (1.0 - 1.5 * SOFT) * slope + (1.0 - SOFT) * cube - (0.5 * SOFT) * inv3
        t = t - 0.5 * squares[h]
        totals.append(jnp.broadcast_to(jnp.sum(t, axis=0, keepdims=True), (8, BLK)))
    return totals


def split3(x):
    high = x.astype(jnp.bfloat16).astype(jnp.float32)
    rest = x - high
    middle = rest.astype(jnp.bfloat16).astype(jnp.float32)
    return high, middle, rest - middle


def walker_kernel(
    pos, spread, table, nuclear, live, out,
    rot, back, grad, left, right, square0, square1, reaches, firsts,
):
    totals = pair_part(pos, rot, back, grad)
    zero = jnp.zeros((8, BLK), jnp.float32)

    column = lax.broadcasted_iota(jnp.int32, (8 * NA, 2 * BLK), 1)
    for e in range(8):
        weights = jnp.where(column % 8 == e, spread[...], 0.0)
        left[e * 128 : e * 128 + 128, :] = weights.astype(jnp.bfloat16)
    for row in range(24, 32):
        right[row * 8 : row * 8 + 8, :] = jnp.full((8, 2 * BLK), 1.0 if row < 27 else 0.0)

    def features(p):
        for h in range(2):
            lanes = slice(h * BLK, h * BLK + BLK)
            x = [pos[p, h, c * 8 : c * 8 + 8, :] for c in range(3)]
            x.append(x[0] * x[0] + x[1] * x[1] + x[2] * x[2])
            tiles = []
            for value in x:
                high, middle, low = split3(value)
                tiles += [high, high, high, middle, middle, low]
            for row, tile in enumerate(tiles):
                right[row * 8 : row * 8 + 8, lanes] = tile

    def squares(square, first, count):
        rows = slice(first * 128, (first + count) * 128)
        factor = right[...].astype(jnp.bfloat16)
        square[rows, :] = jnp.dot(left[rows, :], factor, preferred_element_type=jnp.float32)

    def orbitals(p, square, carry, first):
        energy, logs, pots = (list(part) for part in carry)
        group = range(first, first + GROUP)
        acc = {(e, h): [zero] * 7 for e in group for h in range(2)}
        for a in range(NA):
            level, share, soft, cx, cy, cz, charge = (table[k, a] for k in range(7))
            for h in range(2):
                lanes = slice(h * BLK, h * BLK + BLK)
                near = []
                for e in group:
                    at = (e * NA + a) * 8
                    sq = square[at : at + 8, lanes]
                    inv = lax.rsqrt(sq)
                    amp = jnp.exp2(level - sq * inv)
                    u = amp * inv
                    s = acc[e, h]
                    acc[e, h] = [
                        s[0] + amp * share,
                        s[1] + amp,
                        s[2] + (u * inv) * ((inv + LN2) * soft),
                        s[3] + u,
                        s[4] + u * cx,
                        s[5] + u * cy,
                        s[6] + u * cz,
                    ]
                    near.append(inv)
                pots[h] = pots[h] + functools.reduce(jnp.add, near) * charge
        for e in group:
            for h in range(2):
                phi, amps, soft, us = acc[e, h][:4]
                u = acc[e, h][4:]
                ratio = 1.0 / phi
                at = [slice(c * 8 + e, c * 8 + e + 1) for c in range(3)]
                j = [jnp.broadcast_to(grad[p, h, at[c], :], (8, BLK)) for c in range(3)]
                reach = jnp.broadcast_to(reaches[p, h, e : e + 1, :], (8, BLK))
                part = (0.5 * LN2) * amps - soft - us * reach
                part = part + (u[0] * j[0] + u[1] * j[1] + u[2] * j[2])
                energy[h] = energy[h] - part * ratio
                logs[h] = logs[h] + jnp.log2(phi)
                for k, value in enumerate((*u, us, ratio)):
                    firsts[h, k, e : e + 1, :] = value[0:1, :]
        return tuple(energy), tuple(logs), tuple(pots)

    def reaching(p, _):
        for h in range(2):
            dots = [
                pos[p, h, c * 8 : c * 8 + 8, :] * grad[p, h, c * 8 : c * 8 + 8, :] for c in range(3)
            ]
            reaches[p, h] = (1.0 + dots[0]) + (dots[1] + dots[2])
        return 0

    lax.fori_loop(0, EB, reaching, 0)

    def drift(p):
        for h in range(2):
            for c in range(3):
                rows = slice(c * 8, c * 8 + 8)
                own = (firsts[h, c] - pos[p, h, rows, :] * firsts[h, 3]) * firsts[h, 4]
                out[p, h, rows, :] = own + grad[p, h, rows, :]

    features(0)
    squares(square0, 0, 8)

    def one_block(p, now, later, carry):
        features(jnp.minimum(p + 1, EB - 1))
        for first in range(0, 8, GROUP):
            squares(later, first, GROUP)
            carry = orbitals(p, now, carry, first)
        drift(p)
        return carry

    def some_blocks(t, carry):
        for k in range(0, 4, 2):
            carry = one_block(4 * t + k, square0, square1, carry)
            carry = one_block(4 * t + k + 1, square1, square0, carry)
        return carry

    energy, logs, pots = lax.fori_loop(
        0, EB // 4, some_blocks, ((zero, zero), (zero, zero), (zero, zero))
    )
    row = lax.broadcasted_iota(jnp.int32, (8, BLK), 0)
    lane = lax.broadcasted_iota(jnp.int32, (8, BLK), 1)
    numerator = jnp.zeros((8, 1), jnp.float32)
    denominator = jnp.zeros((8, 1), jnp.float32)
    local = []
    for h in range(2):
        e = (energy[h] - pots[h] + totals[h] + nuclear[...]) * (1.0 / NE)
        weight = jnp.exp2(2.0 * (logs[h] - jnp.broadcast_to(logs[h][0:1, :], (8, BLK))))
        weight = weight * jnp.broadcast_to(live[h : h + 1, :], (8, BLK))
        numerator = numerator + jnp.sum(weight * e, axis=1, keepdims=True)
        denominator = denominator + jnp.sum(weight, axis=1, keepdims=True)
        local.append(e)
    placed = jnp.where(lane == row, numerator, 0.0) + jnp.where(lane == row + 8, denominator, 0.0)
    placed = jnp.broadcast_to(jnp.sum(placed, axis=0, keepdims=True), (8, BLK))
    for h in range(2):
        first = jnp.broadcast_to(local[h][0:1, :], (8, BLK))
        for half in range(2):
            e = local[h] if half == 0 else roll8(local[h], 4)
            tile = jnp.where(row < 4, e, jnp.where(row == 4, first, placed))
            for q in range(8):
                out[half * 8 + q, h, 24:32, :] = tile


def walker_step(whole, spread, table, nuclear, live):
    vmem = pl.BlockSpec(memory_space=pltpu.VMEM)
    rows, width = 8 * NA * 8, 2 * BLK
    return pl.pallas_call(
        walker_kernel,
        out_shape=jax.ShapeDtypeStruct((EB, 2, 32, BLK), jnp.float32),
        in_specs=[vmem] * 5,
        out_specs=vmem,
        scratch_shapes=[
            pltpu.VMEM((EB, 2, 8, 24, BLK), jnp.float32),
            pltpu.VMEM((EB, 2, 8, 24, BLK), jnp.float32),
            pltpu.VMEM((EB, 2, 24, BLK), jnp.float32),
            pltpu.VMEM((rows, width), jnp.bfloat16),
            pltpu.VMEM((width, width), jnp.float32),
            pltpu.VMEM((rows, width), jnp.float32),
            pltpu.VMEM((rows, width), jnp.float32),
            pltpu.VMEM((EB, 2, 8, BLK), jnp.float32),
            pltpu.VMEM((2, 5, 8, BLK), jnp.float32),
        ],
        compiler_params=pltpu.CompilerParams(vmem_limit_bytes=24 * 1024 * 1024),
        name="walker_step",
    )(whole, spread, table, nuclear, live)


def pack_kernel(picked, returned, base, live, send, energy):
    sums = returned[0, 29:30, :]
    for p in range(1, EB):
        sums = sums + returned[2 * p, 29:30, :]
    for b in range(2 * EB):
        energy[:, b * BLK : (b + 1) * BLK] = returned[b, 24:28, :]

    def one_peer(peer, _):
        for k in range(CAP):
            b = picked[peer * CAP + k]
            for c in range(3):
                send[peer, k * 24 + c * 8 : k * 24 + c * 8 + 8, :] = (
                    base[b, c * 8 : c * 8 + 8, :] + TIME_STEP * returned[b, c * 8 : c * 8 + 8, :]
                )
            alive = live[pl.ds(b, 1), :]
            level = returned[b, 28:29, :] - jnp.log(alive)
            send[peer, 96 + k : 97 + k, :] = jnp.where(alive > 0.0, level, 3.0e38)
        send[peer, 100:101, :] = sums
        send[peer, 101:104, :] = jnp.zeros((3, BLK), jnp.float32)
        return 0

    lax.fori_loop(0, send.shape[0], one_peer, 0)


def pack_step(picked, returned, base, live, peers):
    vmem = pl.BlockSpec(memory_space=pltpu.VMEM)
    return pl.pallas_call(
        pack_kernel,
        out_shape=(
            jax.ShapeDtypeStruct((peers, PEER_ROWS, BLK), jnp.float32),
            jax.ShapeDtypeStruct((NG // 2, 2 * EB * BLK), jnp.float32),
        ),
        in_specs=[pl.BlockSpec(memory_space=pltpu.SMEM)] + [vmem] * 3,
        out_specs=(vmem, vmem),
        compiler_params=pltpu.CompilerParams(vmem_limit_bytes=8 * 1024 * 1024),
        name="pack_step",
    )(picked, returned, base, live)


def place_kernel(slots, half, received, moved, weights, estimate):
    sums = received[0, 100:101, :]
    for peer in range(1, received.shape[0]):
        sums = sums + received[peer, 100:101, :]
    sums = jnp.broadcast_to(sums, (8, BLK))
    ratio = sums / pltpu.roll(sums, BLK - 8, axis=1)
    lane = lax.broadcasted_iota(jnp.int32, (8, BLK), 1)
    reference = jnp.sum(jnp.where(lane == 0, ratio, 0.0), axis=1, keepdims=True)[0:1, :]
    own = jnp.where(half[0] == 0, ratio, pltpu.roll(ratio, BLK - 4, axis=1))
    estimate[...] = own[0:1, 0:4]
    for d in range(weights.shape[0]):
        peer, k = slots[d] // CAP, slots[d] % CAP
        for c in range(3):
            at = pl.multiple_of(k * 24 + c * 8, 8)
            moved[c, :, d * BLK : (d + 1) * BLK] = received[peer, pl.ds(at, 8), :]
        level = received[peer, pl.ds(96 + k, 1), :]
        weights[d : d + 1, :] = jnp.exp(-(level - reference))


def place_step(slots, half, received):
    vmem = pl.BlockSpec(memory_space=pltpu.VMEM)
    smem = pl.BlockSpec(memory_space=pltpu.SMEM)
    blocks = slots.shape[0]
    return pl.pallas_call(
        place_kernel,
        out_shape=(
            jax.ShapeDtypeStruct((3, 8, blocks * BLK), jnp.float32),
            jax.ShapeDtypeStruct((blocks, BLK), jnp.float32),
            jax.ShapeDtypeStruct((1, NG // 2), jnp.float32),
        ),
        in_specs=[smem, smem, vmem],
        out_specs=(vmem, vmem, vmem),
        compiler_params=pltpu.CompilerParams(vmem_limit_bytes=8 * 1024 * 1024),
        name="place_step",
    )(slots, half, received)


def nuclear_repulsion(centers, charges):
    offsets = centers[:, :, None, :] - centers[:, None, :, :]
    identity = jnp.eye(NA, dtype=jnp.float32)
    distance = jnp.sqrt(jnp.sum(offsets * offsets, axis=3) + identity)
    product = charges[:, None] * charges[None, :] * (1.0 - identity)
    return 0.5 * jnp.sum(product / distance, axis=(1, 2))


def nucleus_tables(centers, charges, decay, coefficients):
    c = jnp.moveaxis(centers, 1, 0)
    k = (decay * LOG2E)[:, None]
    k2 = k * k
    scale = decay[:, None] * k
    ones = jnp.ones((NA, NG), jnp.float32)

    def thirds(x):
        high = lax.reduce_precision(x, 8, 7)
        rest = x - high
        middle = lax.reduce_precision(rest, 8, 7)
        return high, middle, rest - middle

    rows = []
    for value in [-2.0 * k2 * c[:, :, d] for d in range(3)] + [k2 * ones]:
        high, middle, low = thirds(value)
        rows += [high, middle, low, high, middle, high]
    rows += list(thirds(k2 * (jnp.sum(c * c, axis=2) + SOFT)))
    rows += [jnp.zeros_like(ones)] * (2 * BLK // 8 - len(rows))
    spread = jnp.stack(rows, axis=-1).reshape(NA * NG, len(rows), 1)
    spread = jnp.broadcast_to(spread, (NA * NG, len(rows), 8)).reshape(NA * NG, 2 * BLK)

    factors = [
        jnp.log2(coefficients[:, None] * scale) * ones,
        ones / scale,
        (0.5 * SOFT) * k2 * ones,
        c[:, :, 0],
        c[:, :, 1],
        c[:, :, 2],
        (charges[:, None] * k) * ones,
    ]
    table = jnp.broadcast_to(jnp.stack(factors)[..., None], (len(factors), NA, NG, BLK))
    return spread, table


def by_blocks(x):
    e, c, w = x.shape
    return x.reshape(e, c, w // BLK, BLK).transpose(2, 1, 0, 3).reshape(w // BLK, c * e, BLK)


def local(
    positions,
    diffusion_noise,
    base_nuclei,
    displacements,
    charges,
    orbital_decay,
    coefficients,
    weights,
    counts,
    branch_source,
):
    blocks_here = counts.shape[0]
    peers = lax.axis_size(GX)
    replica = lax.axis_index("gz")
    member = lax.axis_index(GZY)
    device = lax.axis_index(GX)

    sent = by_blocks(positions)
    whole = lax.all_to_all(sent.reshape(EB, 2, 24, BLK), GZY, 0, 0, tiled=True)

    base = sent + STEP_ROOT * by_blocks(diffusion_noise)
    centers = base_nuclei[None, :, :] + displacements
    spread, table = nucleus_tables(centers, charges, orbital_decay, coefficients)
    nuclear = jnp.broadcast_to(nuclear_repulsion(centers, charges)[:, None], (NG, BLK))
    live = jnp.where(
        jnp.arange(BLK, dtype=jnp.int32)[None, :] < counts[:, None],
        weights.reshape(blocks_here, BLK),
        0.0,
    )
    own_live = lax.dynamic_slice_in_dim(live, member * 2, 2, 0)

    block_range = jnp.arange(blocks_here, dtype=jnp.int32)
    total = branch_source.shape[0]
    own_ids = device * blocks_here + block_range
    matches = (branch_source[None, :] == own_ids[:, None]).astype(jnp.int32)
    dest_slot = jnp.sum(matches * jnp.arange(total, dtype=jnp.int32)[None, :], axis=1)
    dest_device = dest_slot // blocks_here
    earlier = (
        (dest_device[None, :] == dest_device[:, None]) & (dest_slot[None, :] < dest_slot[:, None])
    ).astype(jnp.int32)
    send_slot = dest_device * CAP + jnp.sum(earlier, axis=1)
    selection = (
        jnp.arange(peers * CAP, dtype=jnp.int32)[:, None] == send_slot[None, :]
    ).astype(jnp.int32)
    picked = jnp.sum(selection * block_range[None, :], axis=1)
    my_sources = lax.dynamic_slice_in_dim(branch_source, device * blocks_here, blocks_here, 0)
    source_device = my_sources // blocks_here
    before = (
        (source_device[None, :] == source_device[:, None])
        & (block_range[None, :] < block_range[:, None])
    ).astype(jnp.int32)
    slots = source_device * CAP + jnp.sum(before, axis=1)

    out = walker_step(whole, spread, table, nuclear, own_live)
    returned = lax.all_to_all(out, GZY, 0, 0, tiled=True).reshape(blocks_here, 32, BLK)
    send, local_energy = pack_step(picked, returned, base, live, peers)
    received = lax.all_to_all(send, GX, 0, 0, tiled=True)
    moved, new_weights, estimate = place_step(slots, replica.reshape(1), received)
    return (local_energy, estimate.reshape(NG // 2), moved.transpose(1, 0, 2), new_weights.reshape(blocks_here * BLK))


def solution(mesh):
    split = Mesh(
        mesh.devices.reshape(mesh.shape["gz"], 4, 4, mesh.shape["gy"]), ("gz", "gx_0", "gx_1", "gy")
    )
    placed = (
        P(("gz", "gy"), None, GX),
        P(("gz", "gy"), None, GX),
        P(),
        P(),
        P(),
        P(),
        P(),
        P(GX),
        P(GX),
        P(),
    )
    return jax.shard_map(
        local,
        mesh=split,
        in_specs=placed,
        out_specs=(P("gz", GX), P("gz"), P(("gz", "gy"), None, GX), P(GX)),
        check_vma=False,
    )
```

```python
import functools
import math

import jax
import jax.numpy as jnp
from jax import lax
from jax.experimental import pallas as pl
from jax.experimental.pallas import tpu as pltpu
from jax.sharding import Mesh
from jax.sharding import PartitionSpec as P

NE = 128
NA = 16
NG = 8
BLK = 128
EB = 16
GROUP = 4
CAP = 4
SLOT_ROWS = 24
PEER_ROWS = CAP * SLOT_ROWS + 8
GX = ("gx_0", "gx_1")
GZY = ("gz", "gy")

SOFT = 0.04
TIME_STEP = 0.01
STEP_ROOT = 0.1
LN2 = math.log(2.0)
LOG2E = 1.0 / LN2

def roll8(x, shift):
    shift %= 8
    return x if shift == 0 else pltpu.roll(x, shift, axis=0)


def pair_part(pos, rot, back, grad):
    zero = jnp.zeros((8, BLK), jnp.float32)

    def prepare(p, _):
        for h in range(2):
            for c in range(3):
                x = pos[p, h, c * 8 : c * 8 + 8, :]
                for s in range(1, 8):
                    rot[p, h, s - 1, c * 8 : c * 8 + 8, :] = roll8(x, -s)
        return 0

    lax.fori_loop(0, EB, prepare, 0)

    def terms(xi, xj, sums, half):
        d = [xi[c] - xj[c] for c in range(3)]
        square = (d[0] * d[0] + d[1] * d[1]) + (d[2] * d[2] + SOFT)
        inv = lax.rsqrt(square)
        p = 1.0 / (square * inv + 1.0)
        p2 = p * p
        slope = p2 * inv
        parts = (inv, slope, p2 * p, (inv * inv) * inv)
        if half:
            parts = tuple(0.5 * part for part in parts)
        return [slope * d[c] for c in range(3)], tuple(a + b for a, b in zip(sums, parts))

    def load3(ref, *at):
        return [ref[(*at, slice(c * 8, c * 8 + 8), slice(None))] for c in range(3)]

    def store3(ref, values, *at):
        for c in range(3):
            ref[(*at, slice(c * 8, c * 8 + 8), slice(None))] = values[c]

    def turned(j, h, s):
        return load3(pos, j, h) if s == 0 else load3(rot, j, h, s - 1)

    def block_pair(i, j, h, xi, gi, sums, fresh=()):
        for s in range(8):
            f, sums = terms(xi, turned(j, h, s), sums, False)
            gi = [gi[c] + f[c] for c in range(3)]
            if s not in fresh:
                b = load3(back, j, h, s)
                f = [b[c] + f[c] for c in range(3)]
            store3(back, f, j, h, s)
        return gi, sums

    def inside(t, sums):
        out = []
        untouched = (0, 4, 5, 6, 7)
        for h in range(2):
            acc = sums[h]
            own = []
            for i in (2 * t, 2 * t + 1):
                xi, gi = load3(pos, i, h), [zero] * 3
                for s in range(1, 5):
                    f, acc = terms(xi, turned(i, h, s), acc, s == 4)
                    gi = [gi[c] + f[c] for c in range(3)]
                    if s < 4:
                        store3(back, f, i, h, s)
                own.append(gi)
            i, j = 2 * t, 2 * t + 1
            for s in untouched:
                store3(back, [zero] * 3, i, h, s)
            gi, acc = block_pair(i, j, h, load3(pos, i, h), own[0], acc, untouched)
            store3(grad, gi, i, h)
            store3(grad, own[1], j, h)
            out.append(acc)
        return tuple(out)

    def across(u, t, sums):
        out = []
        for h in range(2):
            acc = sums[h]
            for i in (2 * u, 2 * u + 1):
                xi, gi = load3(pos, i, h), load3(grad, i, h)
                for j in (2 * t, 2 * t + 1):
                    gi, acc = block_pair(i, j, h, xi, gi, acc)
                store3(grad, gi, i, h)
            out.append(acc)
        return tuple(out)

    def outer(t, sums):
        sums = inside(t, sums)
        return lax.fori_loop(0, t, lambda u, carry: across(u, t, carry), sums)

    start = ((zero,) * 4, (zero,) * 4)
    sums = lax.fori_loop(0, EB // 2, outer, start)

    def finish(p, squares):
        out = []
        for h in range(2):
            acc = squares[h]
            for c in range(3):
                g = grad[p, h, c * 8 : c * 8 + 8, :]
                for s in range(8):
                    g = g - roll8(back[p, h, s, c * 8 : c * 8 + 8, :], s)
                g = 0.5 * g
                grad[p, h, c * 8 : c * 8 + 8, :] = g
                acc = acc + g * g
            out.append(acc)
        return tuple(out)

    squares = lax.fori_loop(0, EB, finish, (zero, zero))
    totals = []
    for h in range(2):
        inv, slope, cube, inv3 = sums[h]
        t = inv - (1.0 - 1.5 * SOFT) * slope + (1.0 - SOFT) * cube - (0.5 * SOFT) * inv3
        t = t - 0.5 * squares[h]
        totals.append(jnp.broadcast_to(jnp.sum(t, axis=0, keepdims=True), (8, BLK)))
    return totals


def split3(x):
    high = x.astype(jnp.bfloat16).astype(jnp.float32)
    rest = x - high
    middle = rest.astype(jnp.bfloat16).astype(jnp.float32)
    return high, middle, rest - middle


def pair_kernel(pos, grad, totals, rot, back):
    for h, total in enumerate(pair_part(pos, rot, back, grad)):
        totals[h] = total


def orbital_kernel(
    pos, grad, totals, spread, table, nuclear, live, out,
    left, right, square0, square1, reaches,
):
    zero = jnp.zeros((8, BLK), jnp.float32)

    column = lax.broadcasted_iota(jnp.int32, (8 * NA, 2 * BLK), 1)
    for e in range(8):
        weights = jnp.where(column % 8 == e, spread[...], 0.0)
        left[e * 128 : e * 128 + 128, :] = weights.astype(jnp.bfloat16)
    for row in range(24, 32):
        right[row * 8 : row * 8 + 8, :] = jnp.full((8, 2 * BLK), 1.0 if row < 27 else 0.0)

    def features(p):
        for h in range(2):
            lanes = slice(h * BLK, h * BLK + BLK)
            x = [pos[p, h, c * 8 : c * 8 + 8, :] for c in range(3)]
            x.append(x[0] * x[0] + x[1] * x[1] + x[2] * x[2])
            tiles = []
            for value in x:
                high, middle, low = split3(value)
                tiles += [high, high, high, middle, middle, low]
            for row, tile in enumerate(tiles):
                right[row * 8 : row * 8 + 8, lanes] = tile

    def squares(square, first, count):
        rows = slice(first * 128, (first + count) * 128)
        factor = right[...].astype(jnp.bfloat16)
        square[rows, :] = jnp.dot(left[rows, :], factor, preferred_element_type=jnp.float32)

    def orbitals(p, square, carry, first):
        energy, logs, pots = (list(part) for part in carry)
        group = range(first, first + GROUP)
        acc = {(e, h): [zero] * 7 for e in group for h in range(2)}
        for a in range(NA):
            level, share, soft, cx, cy, cz, charge = (table[k, a] for k in range(7))
            for h in range(2):
                lanes = slice(h * BLK, h * BLK + BLK)
                near = []
                for e in group:
                    at = (e * NA + a) * 8
                    sq = square[at : at + 8, lanes]
                    inv = lax.rsqrt(sq)
                    amp = jnp.exp2(level - sq * inv)
                    u = amp * inv
                    s = acc[e, h]
                    acc[e, h] = [
                        s[0] + amp * share,
                        s[1] + amp,
                        s[2] + (u * inv) * ((inv + LN2) * soft),
                        s[3] + u,
                        s[4] + u * cx,
                        s[5] + u * cy,
                        s[6] + u * cz,
                    ]
                    near.append(inv)
                pots[h] = pots[h] + functools.reduce(jnp.add, near) * charge
        for e in group:
            for h in range(2):
                phi, amps, soft, us = acc[e, h][:4]
                u = acc[e, h][4:]
                ratio = 1.0 / phi
                at = [slice(c * 8 + e, c * 8 + e + 1) for c in range(3)]
                j = [jnp.broadcast_to(grad[p, h, at[c], :], (8, BLK)) for c in range(3)]
                reach = jnp.broadcast_to(reaches[p, h, e : e + 1, :], (8, BLK))
                part = (0.5 * LN2) * amps - soft - us * reach
                part = part + (u[0] * j[0] + u[1] * j[1] + u[2] * j[2])
                energy[h] = energy[h] - part * ratio
                logs[h] = logs[h] + jnp.log2(phi)
        return tuple(energy), tuple(logs), tuple(pots)

    def reaching(p, _):
        for h in range(2):
            dots = [
                pos[p, h, c * 8 : c * 8 + 8, :] * grad[p, h, c * 8 : c * 8 + 8, :] for c in range(3)
            ]
            reaches[p, h] = (1.0 + dots[0]) + (dots[1] + dots[2])
        return 0

    lax.fori_loop(0, EB, reaching, 0)

    features(0)
    squares(square0, 0, 8)

    def one_block(p, now, later, carry):
        features(jnp.minimum(p + 1, EB - 1))
        for first in range(0, 8, GROUP):
            squares(later, first, GROUP)
            carry = orbitals(p, now, carry, first)
        return carry

    def some_blocks(t, carry):
        for k in range(0, 4, 2):
            carry = one_block(4 * t + k, square0, square1, carry)
            carry = one_block(4 * t + k + 1, square1, square0, carry)
        return carry

    energy, logs, pots = lax.fori_loop(
        0, EB // 4, some_blocks, ((zero, zero), (zero, zero), (zero, zero))
    )
    row = lax.broadcasted_iota(jnp.int32, (8, BLK), 0)
    lane = lax.broadcasted_iota(jnp.int32, (8, BLK), 1)
    numerator = jnp.zeros((8, 1), jnp.float32)
    denominator = jnp.zeros((8, 1), jnp.float32)
    local = []
    for h in range(2):
        e = (energy[h] - pots[h] + totals[h] + nuclear[...]) * (1.0 / NE)
        weight = jnp.exp2(2.0 * (logs[h] - jnp.broadcast_to(logs[h][0:1, :], (8, BLK))))
        weight = weight * jnp.broadcast_to(live[h : h + 1, :], (8, BLK))
        numerator = numerator + jnp.sum(weight * e, axis=1, keepdims=True)
        denominator = denominator + jnp.sum(weight, axis=1, keepdims=True)
        local.append(e)
    placed = jnp.where(lane == row, numerator, 0.0) + jnp.where(lane == row + 8, denominator, 0.0)
    placed = jnp.broadcast_to(jnp.sum(placed, axis=0, keepdims=True), (8, BLK))
    firsts = [jnp.broadcast_to(local[h][0:1, :], (8, BLK)) for h in range(2)]
    rest = jnp.where(row == 0, firsts[0], jnp.where(row == 1, firsts[1], placed))
    for q in range(EB):
        low, high = local if q < EB // 2 else (roll8(local[0], 4), roll8(local[1], 4))
        out[q, 0:8, :] = jnp.where(row < 4, low, roll8(high, 4))
        out[q, 8:16, :] = rest


def pair_step(whole):
    vmem = pl.BlockSpec(memory_space=pltpu.VMEM)
    return pl.pallas_call(
        pair_kernel,
        out_shape=(
            jax.ShapeDtypeStruct((EB, 2, 24, BLK), jnp.float32),
            jax.ShapeDtypeStruct((2, 8, BLK), jnp.float32),
        ),
        in_specs=[vmem],
        out_specs=(vmem, vmem),
        scratch_shapes=[
            pltpu.VMEM((EB, 2, 7, 24, BLK), jnp.float32),
            pltpu.VMEM((EB, 2, 8, 24, BLK), jnp.float32),
        ],
        compiler_params=pltpu.CompilerParams(vmem_limit_bytes=16 * 1024 * 1024),
        cost_estimate=pl.CostEstimate(
            flops=EB * EB * BLK * 2 * 32 * 32, transcendentals=0, bytes_accessed=1 << 20
        ),
        name="pair_step",
    )(whole)


def orbital_step(whole, grad, totals, spread, table, nuclear, live):
    vmem = pl.BlockSpec(memory_space=pltpu.VMEM)
    rows, width = 8 * NA * 8, 2 * BLK
    return pl.pallas_call(
        orbital_kernel,
        out_shape=jax.ShapeDtypeStruct((EB, 16, BLK), jnp.float32),
        in_specs=[vmem] * 7,
        out_specs=vmem,
        scratch_shapes=[
            pltpu.VMEM((rows, width), jnp.bfloat16),
            pltpu.VMEM((width, width), jnp.float32),
            pltpu.VMEM((rows, width), jnp.float32),
            pltpu.VMEM((rows, width), jnp.float32),
            pltpu.VMEM((EB, 2, 8, BLK), jnp.float32),
        ],
        compiler_params=pltpu.CompilerParams(vmem_limit_bytes=16 * 1024 * 1024),
        cost_estimate=pl.CostEstimate(
            flops=EB * 8 * NA * NG * BLK * 2 * 32 * 2, transcendentals=0, bytes_accessed=1 << 20
        ),
        name="orbital_step",
    )(whole, grad, totals, spread, table, nuclear, live)


def own_kernel(scalars, positions, noise, base):
    wide = 4 * BLK

    def four(t, _):
        at = pl.multiple_of(t * wide, wide)
        r = [positions[c, :, pl.ds(at, wide)] for c in range(3)]
        phi = jnp.zeros((8, wide), jnp.float32)
        grad = [phi, phi, phi]
        for a in range(NA):
            v = [r[c] - scalars[c, a] for c in range(3)]
            square = (v[0] * v[0] + v[1] * v[1]) + (v[2] * v[2] + SOFT)
            inv = lax.rsqrt(square)
            amp = jnp.exp2(scalars[4, a] - scalars[3, a] * (square * inv))
            u = amp * inv
            phi = phi + amp * scalars[5, a]
            grad = [grad[c] + u * v[c] for c in range(3)]
        step = TIME_STEP / phi
        for c in range(3):
            moved = r[c] + STEP_ROOT * noise[c, :, pl.ds(at, wide)] - step * grad[c]
            for k in range(4):
                base[t * 4 + k, c * 8 : c * 8 + 8, :] = moved[:, k * BLK : (k + 1) * BLK]
        return 0

    lax.fori_loop(0, base.shape[0] // 4, four, 0)


def own_step(scalars, positions, noise):
    vmem = pl.BlockSpec(memory_space=pltpu.VMEM)
    blocks = positions.shape[2] // BLK
    return pl.pallas_call(
        own_kernel,
        out_shape=jax.ShapeDtypeStruct((blocks, 24, BLK), jnp.float32),
        in_specs=[pl.BlockSpec(memory_space=pltpu.SMEM), vmem, vmem],
        out_specs=vmem,
        compiler_params=pltpu.CompilerParams(vmem_limit_bytes=8 * 1024 * 1024),
        name="own_step",
    )(scalars, positions, noise)


def blocks_kernel(picked, returned, base, send):
    def one_peer(peer, _):
        for k in range(CAP):
            b = picked[peer * CAP + k]
            for c in range(3):
                send[peer, k * 24 + c * 8 : k * 24 + c * 8 + 8, :] = (
                    base[b, c * 8 : c * 8 + 8, :] + TIME_STEP * returned[b, c * 8 : c * 8 + 8, :]
                )
        send[peer, 96:104, :] = jnp.zeros((8, BLK), jnp.float32)
        return 0

    lax.fori_loop(0, send.shape[0], one_peer, 0)


def blocks_step(picked, returned, base, peers):
    vmem = pl.BlockSpec(memory_space=pltpu.VMEM)
    return pl.pallas_call(
        blocks_kernel,
        out_shape=jax.ShapeDtypeStruct((peers, PEER_ROWS, BLK), jnp.float32),
        in_specs=[pl.BlockSpec(memory_space=pltpu.SMEM)] + [vmem] * 2,
        out_specs=vmem,
        compiler_params=pltpu.CompilerParams(vmem_limit_bytes=8 * 1024 * 1024),
        cost_estimate=pl.CostEstimate(flops=1 << 24, transcendentals=0, bytes_accessed=1 << 21),
        name="blocks_step",
    )(picked, returned, base)


def levels_kernel(picked, energies, live, _, send, energy, tiles, done):
    sums = energies[0, 10:11, :]
    for p in range(1, EB):
        sums = sums + energies[p, 10:11, :]
    peers = tiles.shape[0]
    for peer in range(peers):
        for k in range(CAP):
            b = picked[peer * CAP + k]
            alive = live[pl.ds(b, 1), :]
            level = energies[b // 2, pl.ds(8 + b % 2, 1), :] - jnp.log(alive)
            tiles[peer, k : k + 1, :] = jnp.where(alive > 0.0, level, 3.0e38)
        tiles[peer, 4:5, :] = sums
        tiles[peer, 5:8, :] = jnp.zeros((3, BLK), jnp.float32)
    copy = pltpu.make_async_copy(tiles, send.at[:, 96:104, :], done)
    copy.start()
    for b in range(2 * EB):
        at = (b % 2) * 4
        energy[:, b * BLK : (b + 1) * BLK] = energies[b // 2, at : at + 4, :]
    copy.wait()


def levels_step(picked, energies, live, send):
    vmem = pl.BlockSpec(memory_space=pltpu.VMEM)
    whole = pl.BlockSpec(memory_space=pl.ANY)
    peers = send.shape[0]
    return pl.pallas_call(
        levels_kernel,
        out_shape=(
            jax.ShapeDtypeStruct(send.shape, jnp.float32),
            jax.ShapeDtypeStruct((NG // 2, 2 * EB * BLK), jnp.float32),
        ),
        in_specs=[pl.BlockSpec(memory_space=pltpu.SMEM), vmem, vmem, whole],
        out_specs=(whole, vmem),
        scratch_shapes=[pltpu.VMEM((peers, 8, BLK), jnp.float32), pltpu.SemaphoreType.DMA],
        input_output_aliases={3: 0},
        compiler_params=pltpu.CompilerParams(vmem_limit_bytes=8 * 1024 * 1024),
        name="levels_step",
    )(picked, energies, live, send)


def place_kernel(slots, half, received, moved, weights, estimate):
    sums = received[0, 100:101, :]
    for peer in range(1, received.shape[0]):
        sums = sums + received[peer, 100:101, :]
    sums = jnp.broadcast_to(sums, (8, BLK))
    ratio = sums / pltpu.roll(sums, BLK - 8, axis=1)
    lane = lax.broadcasted_iota(jnp.int32, (8, BLK), 1)
    reference = jnp.sum(jnp.where(lane == 0, ratio, 0.0), axis=1, keepdims=True)[0:1, :]
    own = jnp.where(half[0] == 0, ratio, pltpu.roll(ratio, BLK - 4, axis=1))
    estimate[...] = own[0:1, 0:4]
    for d in range(weights.shape[0]):
        peer, k = slots[d] // CAP, slots[d] % CAP
        for c in range(3):
            at = pl.multiple_of(k * 24 + c * 8, 8)
            moved[c, :, d * BLK : (d + 1) * BLK] = received[peer, pl.ds(at, 8), :]
        level = received[peer, pl.ds(96 + k, 1), :]
        weights[d : d + 1, :] = jnp.exp(-(level - reference))


def place_step(slots, half, received):
    vmem = pl.BlockSpec(memory_space=pltpu.VMEM)
    smem = pl.BlockSpec(memory_space=pltpu.SMEM)
    blocks = slots.shape[0]
    return pl.pallas_call(
        place_kernel,
        out_shape=(
            jax.ShapeDtypeStruct((3, 8, blocks * BLK), jnp.float32),
            jax.ShapeDtypeStruct((blocks, BLK), jnp.float32),
            jax.ShapeDtypeStruct((1, NG // 2), jnp.float32),
        ),
        in_specs=[smem, smem, vmem],
        out_specs=(vmem, vmem, vmem),
        compiler_params=pltpu.CompilerParams(vmem_limit_bytes=8 * 1024 * 1024),
        name="place_step",
    )(slots, half, received)


def nuclear_repulsion(centers, charges):
    offsets = centers[:, :, None, :] - centers[:, None, :, :]
    identity = jnp.eye(NA, dtype=jnp.float32)
    distance = jnp.sqrt(jnp.sum(offsets * offsets, axis=3) + identity)
    product = charges[:, None] * charges[None, :] * (1.0 - identity)
    return 0.5 * jnp.sum(product / distance, axis=(1, 2))


def nucleus_tables(centers, charges, decay, coefficients):
    c = jnp.moveaxis(centers, 1, 0)
    k = (decay * LOG2E)[:, None]
    k2 = k * k
    scale = decay[:, None] * k
    ones = jnp.ones((NA, NG), jnp.float32)

    def thirds(x):
        high = lax.reduce_precision(x, 8, 7)
        rest = x - high
        middle = lax.reduce_precision(rest, 8, 7)
        return high, middle, rest - middle

    rows = []
    for value in [-2.0 * k2 * c[:, :, d] for d in range(3)] + [k2 * ones]:
        high, middle, low = thirds(value)
        rows += [high, middle, low, high, middle, high]
    rows += list(thirds(k2 * (jnp.sum(c * c, axis=2) + SOFT)))
    rows += [jnp.zeros_like(ones)] * (2 * BLK // 8 - len(rows))
    spread = jnp.stack(rows, axis=-1).reshape(NA * NG, len(rows), 1)
    spread = jnp.broadcast_to(spread, (NA * NG, len(rows), 8)).reshape(NA * NG, 2 * BLK)

    factors = [
        jnp.log2(coefficients[:, None] * scale) * ones,
        ones / scale,
        (0.5 * SOFT) * k2 * ones,
        c[:, :, 0],
        c[:, :, 1],
        c[:, :, 2],
        (charges[:, None] * k) * ones,
    ]
    table = jnp.broadcast_to(jnp.stack(factors)[..., None], (len(factors), NA, NG, BLK))
    return spread, table


def by_blocks(x):
    e, c, w = x.shape
    return x.reshape(e, c, w // BLK, BLK).transpose(2, 1, 0, 3).reshape(w // BLK, c * e, BLK)


def local(
    positions,
    diffusion_noise,
    base_nuclei,
    displacements,
    charges,
    orbital_decay,
    coefficients,
    weights,
    counts,
    branch_source,
):
    blocks_here = counts.shape[0]
    peers = lax.axis_size(GX)
    replica = lax.axis_index("gz")
    member = lax.axis_index(GZY)
    device = lax.axis_index(GX)

    sent = by_blocks(positions)
    whole = lax.all_to_all(sent.reshape(EB, 2, 24, BLK), GZY, 0, 0, tiled=True)

    centers = base_nuclei[None, :, :] + displacements
    first = centers[0]
    rate = orbital_decay * LOG2E
    level = jnp.log2(coefficients * orbital_decay)
    scalars = jnp.stack([first[:, 0], first[:, 1], first[:, 2], rate, level, 1.0 / orbital_decay])
    base = own_step(scalars, positions.transpose(1, 0, 2), diffusion_noise.transpose(1, 0, 2))
    spread, table = nucleus_tables(centers, charges, orbital_decay, coefficients)
    nuclear = jnp.broadcast_to(nuclear_repulsion(centers, charges)[:, None], (NG, BLK))
    live = jnp.where(
        jnp.arange(BLK, dtype=jnp.int32)[None, :] < counts[:, None],
        weights.reshape(blocks_here, BLK),
        0.0,
    )
    own_live = lax.dynamic_slice_in_dim(live, member * 2, 2, 0)

    block_range = jnp.arange(blocks_here, dtype=jnp.int32)
    total = branch_source.shape[0]
    own_ids = device * blocks_here + block_range
    matches = (branch_source[None, :] == own_ids[:, None]).astype(jnp.int32)
    dest_slot = jnp.sum(matches * jnp.arange(total, dtype=jnp.int32)[None, :], axis=1)
    dest_device = dest_slot // blocks_here
    earlier = (
        (dest_device[None, :] == dest_device[:, None]) & (dest_slot[None, :] < dest_slot[:, None])
    ).astype(jnp.int32)
    send_slot = dest_device * CAP + jnp.sum(earlier, axis=1)
    selection = (
        jnp.arange(peers * CAP, dtype=jnp.int32)[:, None] == send_slot[None, :]
    ).astype(jnp.int32)
    picked = jnp.sum(selection * block_range[None, :], axis=1)
    my_sources = lax.dynamic_slice_in_dim(branch_source, device * blocks_here, blocks_here, 0)
    source_device = my_sources // blocks_here
    before = (
        (source_device[None, :] == source_device[:, None])
        & (block_range[None, :] < block_range[:, None])
    ).astype(jnp.int32)
    slots = source_device * CAP + jnp.sum(before, axis=1)

    whole, base, spread, table, nuclear, own_live, picked = lax.optimization_barrier(
        (whole, base, spread, table, nuclear, own_live, picked)
    )
    grad, totals = pair_step(whole)
    returned = lax.all_to_all(grad, GZY, 0, 0, tiled=True).reshape(blocks_here, 24, BLK)
    out = orbital_step(whole, grad, totals, spread, table, nuclear, own_live)
    returned, out = lax.optimization_barrier((returned, out))
    energies = lax.all_to_all(out, GZY, 0, 0, tiled=True)
    send = blocks_step(picked, returned, base, peers)
    send, local_energy = levels_step(picked, energies, live, send)
    received = lax.all_to_all(send, GX, 0, 0, tiled=True)
    moved, new_weights, estimate = place_step(slots, replica.reshape(1), received)
    return (local_energy, estimate.reshape(NG // 2), moved.transpose(1, 0, 2), new_weights.reshape(blocks_here * BLK))


def solution(mesh):
    split = Mesh(
        mesh.devices.reshape(mesh.shape["gz"], 4, 4, mesh.shape["gy"]), ("gz", "gx_0", "gx_1", "gy")
    )
    placed = (
        P(("gz", "gy"), None, GX),
        P(("gz", "gy"), None, GX),
        P(),
        P(),
        P(),
        P(),
        P(),
        P(GX),
        P(GX),
        P(),
    )
    return jax.shard_map(
        local,
        mesh=split,
        in_specs=placed,
        out_specs=(P("gz", GX), P("gz"), P(("gz", "gy"), None, GX), P(GX)),
        check_vma=False,
    )
```

```python
import functools
import math

import jax
import jax.numpy as jnp
from jax import lax
from jax.experimental import pallas as pl
from jax.experimental.pallas import tpu as pltpu
from jax.sharding import Mesh
from jax.sharding import PartitionSpec as P

NE = 128
NA = 16
NG = 8
BLK = 128
EB = 16
GROUP = 4
CAP = 4
SLOT_ROWS = 24
PEER_ROWS = CAP * SLOT_ROWS + 8
GX = ("gx_0", "gx_1")
GZY = ("gz", "gy")

SOFT = 0.04
TIME_STEP = 0.01
STEP_ROOT = 0.1
LN2 = math.log(2.0)
LOG2E = 1.0 / LN2

def roll8(x, shift):
    shift %= 8
    return x if shift == 0 else pltpu.roll(x, shift, axis=0)


def pair_part(pos, rot, back, grad):
    zero = jnp.zeros((8, BLK), jnp.float32)

    def prepare(p, _):
        for h in range(2):
            for c in range(3):
                x = pos[p, h, c * 8 : c * 8 + 8, :]
                for s in range(1, 8):
                    rot[p, h, s - 1, c * 8 : c * 8 + 8, :] = roll8(x, -s)
        return 0

    lax.fori_loop(0, EB, prepare, 0)

    def terms(xi, xj, sums, half):
        d = [xi[c] - xj[c] for c in range(3)]
        square = (d[0] * d[0] + d[1] * d[1]) + (d[2] * d[2] + SOFT)
        inv = lax.rsqrt(square)
        p = 1.0 / (square * inv + 1.0)
        p2 = p * p
        slope = p2 * inv
        parts = (inv, slope, p2 * p, (inv * inv) * inv)
        if half:
            parts = tuple(0.5 * part for part in parts)
        return [slope * d[c] for c in range(3)], tuple(a + b for a, b in zip(sums, parts))

    def load3(ref, *at):
        return [ref[(*at, slice(c * 8, c * 8 + 8), slice(None))] for c in range(3)]

    def store3(ref, values, *at):
        for c in range(3):
            ref[(*at, slice(c * 8, c * 8 + 8), slice(None))] = values[c]

    def turned(j, h, s):
        return load3(pos, j, h) if s == 0 else load3(rot, j, h, s - 1)

    def block_pair(i, j, h, xi, gi, sums, fresh=()):
        for s in range(8):
            f, sums = terms(xi, turned(j, h, s), sums, False)
            gi = [gi[c] + f[c] for c in range(3)]
            if s not in fresh:
                b = load3(back, j, h, s)
                f = [b[c] + f[c] for c in range(3)]
            store3(back, f, j, h, s)
        return gi, sums

    def inside(t, sums):
        out = []
        untouched = (0, 4, 5, 6, 7)
        for h in range(2):
            acc = sums[h]
            own = []
            for i in (2 * t, 2 * t + 1):
                xi, gi = load3(pos, i, h), [zero] * 3
                for s in range(1, 5):
                    f, acc = terms(xi, turned(i, h, s), acc, s == 4)
                    gi = [gi[c] + f[c] for c in range(3)]
                    if s < 4:
                        store3(back, f, i, h, s)
                own.append(gi)
            i, j = 2 * t, 2 * t + 1
            for s in untouched:
                store3(back, [zero] * 3, i, h, s)
            gi, acc = block_pair(i, j, h, load3(pos, i, h), own[0], acc, untouched)
            store3(grad, gi, i, h)
            store3(grad, own[1], j, h)
            out.append(acc)
        return tuple(out)

    def across(u, t, sums):
        out = []
        for h in range(2):
            acc = sums[h]
            for i in (2 * u, 2 * u + 1):
                xi, gi = load3(pos, i, h), load3(grad, i, h)
                for j in (2 * t, 2 * t + 1):
                    gi, acc = block_pair(i, j, h, xi, gi, acc)
                store3(grad, gi, i, h)
            out.append(acc)
        return tuple(out)

    def outer(t, sums):
        sums = inside(t, sums)
        return lax.fori_loop(0, t, lambda u, carry: across(u, t, carry), sums)

    start = ((zero,) * 4, (zero,) * 4)
    sums = lax.fori_loop(0, EB // 2, outer, start)

    def finish(p, squares):
        out = []
        for h in range(2):
            acc = squares[h]
            for c in range(3):
                g = grad[p, h, c * 8 : c * 8 + 8, :]
                for s in range(8):
                    g = g - roll8(back[p, h, s, c * 8 : c * 8 + 8, :], s)
                g = 0.5 * g
                grad[p, h, c * 8 : c * 8 + 8, :] = g
                acc = acc + g * g
            out.append(acc)
        return tuple(out)

    squares = lax.fori_loop(0, EB, finish, (zero, zero))
    totals = []
    for h in range(2):
        inv, slope, cube, inv3 = sums[h]
        t = inv - (1.0 - 1.5 * SOFT) * slope + (1.0 - SOFT) * cube - (0.5 * SOFT) * inv3
        t = t - 0.5 * squares[h]
        totals.append(jnp.broadcast_to(jnp.sum(t, axis=0, keepdims=True), (8, BLK)))
    return totals


def split3(x):
    high = x.astype(jnp.bfloat16).astype(jnp.float32)
    rest = x - high
    middle = rest.astype(jnp.bfloat16).astype(jnp.float32)
    return high, middle, rest - middle


def walker_kernel(
    pos, spread, table, nuclear, live, out,
    rot, back, grad, left, right, square0, square1, reaches, firsts,
):
    totals = pair_part(pos, rot, back, grad)
    zero = jnp.zeros((8, BLK), jnp.float32)

    column = lax.broadcasted_iota(jnp.int32, (8 * NA, 2 * BLK), 1)
    for e in range(8):
        weights = jnp.where(column % 8 == e, spread[...], 0.0)
        left[e * 128 : e * 128 + 128, :] = weights.astype(jnp.bfloat16)
    for row in range(24, 32):
        right[row * 8 : row * 8 + 8, :] = jnp.full((8, 2 * BLK), 1.0 if row < 27 else 0.0)

    def features(p):
        for h in range(2):
            lanes = slice(h * BLK, h * BLK + BLK)
            x = [pos[p, h, c * 8 : c * 8 + 8, :] for c in range(3)]
            x.append(x[0] * x[0] + x[1] * x[1] + x[2] * x[2])
            tiles = []
            for value in x:
                high, middle, low = split3(value)
                tiles += [high, high, high, middle, middle, low]
            for row, tile in enumerate(tiles):
                right[row * 8 : row * 8 + 8, lanes] = tile

    def squares(square, first, count):
        rows = slice(first * 128, (first + count) * 128)
        factor = right[...].astype(jnp.bfloat16)
        square[rows, :] = jnp.dot(left[rows, :], factor, preferred_element_type=jnp.float32)

    def orbitals(p, square, carry, first):
        energy, logs, pots = (list(part) for part in carry)
        group = range(first, first + GROUP)
        acc = {(e, h): [zero] * 7 for e in group for h in range(2)}
        for a in range(NA):
            level, share, soft, cx, cy, cz, charge = (table[k, a] for k in range(7))
            for h in range(2):
                lanes = slice(h * BLK, h * BLK + BLK)
                near = []
                for e in group:
                    at = (e * NA + a) * 8
                    sq = square[at : at + 8, lanes]
                    inv = lax.rsqrt(sq)
                    amp = jnp.exp2(level - sq * inv)
                    u = amp * inv
                    s = acc[e, h]
                    acc[e, h] = [
                        s[0] + amp * share,
                        s[1] + amp,
                        s[2] + (u * inv) * ((inv + LN2) * soft),
                        s[3] + u,
                        s[4] + u * cx,
                        s[5] + u * cy,
                        s[6] + u * cz,
                    ]
                    near.append(inv)
                pots[h] = pots[h] + functools.reduce(jnp.add, near) * charge
        for e in group:
            for h in range(2):
                phi, amps, soft, us = acc[e, h][:4]
                u = acc[e, h][4:]
                ratio = 1.0 / phi
                at = [slice(c * 8 + e, c * 8 + e + 1) for c in range(3)]
                j = [jnp.broadcast_to(grad[p, h, at[c], :], (8, BLK)) for c in range(3)]
                reach = jnp.broadcast_to(reaches[p, h, e : e + 1, :], (8, BLK))
                part = (0.5 * LN2) * amps - soft - us * reach
                part = part + (u[0] * j[0] + u[1] * j[1] + u[2] * j[2])
                energy[h] = energy[h] - part * ratio
                logs[h] = logs[h] + jnp.log2(phi)
                for k, value in enumerate((*u, us, ratio)):
                    firsts[h, k, e : e + 1, :] = value[0:1, :]
        return tuple(energy), tuple(logs), tuple(pots)

    def reaching(p, _):
        for h in range(2):
            dots = [
                pos[p, h, c * 8 : c * 8 + 8, :] * grad[p, h, c * 8 : c * 8 + 8, :] for c in range(3)
            ]
            reaches[p, h] = (1.0 + dots[0]) + (dots[1] + dots[2])
        return 0

    lax.fori_loop(0, EB, reaching, 0)

    def drift(p):
        for h in range(2):
            for c in range(3):
                rows = slice(c * 8, c * 8 + 8)
                own = (firsts[h, c] - pos[p, h, rows, :] * firsts[h, 3]) * firsts[h, 4]
                out[p, h, rows, :] = own + grad[p, h, rows, :]

    features(0)
    squares(square0, 0, 8)

    def one_block(p, now, later, carry):
        features(jnp.minimum(p + 1, EB - 1))
        for first in range(0, 8, GROUP):
            squares(later, first, GROUP)
            carry = orbitals(p, now, carry, first)
        drift(p)
        return carry

    def some_blocks(t, carry):
        for k in range(0, 4, 2):
            carry = one_block(4 * t + k, square0, square1, carry)
            carry = one_block(4 * t + k + 1, square1, square0, carry)
        return carry

    energy, logs, pots = lax.fori_loop(
        0, EB // 4, some_blocks, ((zero, zero), (zero, zero), (zero, zero))
    )
    row = lax.broadcasted_iota(jnp.int32, (8, BLK), 0)
    lane = lax.broadcasted_iota(jnp.int32, (8, BLK), 1)
    numerator = jnp.zeros((8, 1), jnp.float32)
    denominator = jnp.zeros((8, 1), jnp.float32)
    local = []
    for h in range(2):
        e = (energy[h] - pots[h] + totals[h] + nuclear[...]) * (1.0 / NE)
        weight = jnp.exp2(2.0 * (logs[h] - jnp.broadcast_to(logs[h][0:1, :], (8, BLK))))
        weight = weight * jnp.broadcast_to(live[h : h + 1, :], (8, BLK))
        numerator = numerator + jnp.sum(weight * e, axis=1, keepdims=True)
        denominator = denominator + jnp.sum(weight, axis=1, keepdims=True)
        local.append(e)
    placed = jnp.where(lane == row, numerator, 0.0) + jnp.where(lane == row + 8, denominator, 0.0)
    placed = jnp.broadcast_to(jnp.sum(placed, axis=0, keepdims=True), (8, BLK))
    for h in range(2):
        first = jnp.broadcast_to(local[h][0:1, :], (8, BLK))
        for half in range(2):
            e = local[h] if half == 0 else roll8(local[h], 4)
            tile = jnp.where(row < 4, e, jnp.where(row == 4, first, placed))
            for q in range(8):
                out[half * 8 + q, h, 24:32, :] = tile


def walker_step(whole, spread, table, nuclear, live):
    vmem = pl.BlockSpec(memory_space=pltpu.VMEM)
    rows, width = 8 * NA * 8, 2 * BLK
    return pl.pallas_call(
        walker_kernel,
        out_shape=jax.ShapeDtypeStruct((EB, 2, 32, BLK), jnp.float32),
        in_specs=[vmem] * 5,
        out_specs=vmem,
        scratch_shapes=[
            pltpu.VMEM((EB, 2, 7, 24, BLK), jnp.float32),
            pltpu.VMEM((EB, 2, 8, 24, BLK), jnp.float32),
            pltpu.VMEM((EB, 2, 24, BLK), jnp.float32),
            pltpu.VMEM((rows, width), jnp.bfloat16),
            pltpu.VMEM((width, width), jnp.float32),
            pltpu.VMEM((rows, width), jnp.float32),
            pltpu.VMEM((rows, width), jnp.float32),
            pltpu.VMEM((EB, 2, 8, BLK), jnp.float32),
            pltpu.VMEM((2, 5, 8, BLK), jnp.float32),
        ],
        compiler_params=pltpu.CompilerParams(vmem_limit_bytes=24 * 1024 * 1024),
        name="walker_step",
    )(whole, spread, table, nuclear, live)


def pack_kernel(picked, returned, base, live, send, energy, held, gone):
    sums = returned[0, 29:30, :]
    for p in range(1, EB):
        sums = sums + returned[2 * p, 29:30, :]
    peers = held.shape[0]

    def leaving(peer):
        return pltpu.make_async_copy(held.at[peer], send.at[peer], gone.at[peer])

    def one_peer(peer, _):
        for k in range(CAP):
            b = picked[peer * CAP + k]
            for c in range(3):
                held[peer, k * 24 + c * 8 : k * 24 + c * 8 + 8, :] = (
                    base[b, c * 8 : c * 8 + 8, :] + TIME_STEP * returned[b, c * 8 : c * 8 + 8, :]
                )
            alive = live[pl.ds(b, 1), :]
            level = returned[b, 28:29, :] - jnp.log(alive)
            held[peer, 96 + k : 97 + k, :] = jnp.where(alive > 0.0, level, 3.0e38)
        held[peer, 100:101, :] = sums
        held[peer, 101:104, :] = jnp.zeros((3, BLK), jnp.float32)
        leaving(peer).start()
        return 0

    lax.fori_loop(0, peers, one_peer, 0)
    for b in range(2 * EB):
        energy[:, b * BLK : (b + 1) * BLK] = returned[b, 24:28, :]
    for peer in range(peers):
        leaving(peer).wait()


def pack_step(picked, returned, base, live, peers):
    vmem = pl.BlockSpec(memory_space=pltpu.VMEM)
    shape = (peers, PEER_ROWS, BLK)
    return pl.pallas_call(
        pack_kernel,
        out_shape=(
            jax.ShapeDtypeStruct(shape, jnp.float32),
            jax.ShapeDtypeStruct((NG // 2, 2 * EB * BLK), jnp.float32),
        ),
        in_specs=[pl.BlockSpec(memory_space=pltpu.SMEM)] + [vmem] * 3,
        out_specs=(pl.BlockSpec(memory_space=pltpu.HBM), vmem),
        scratch_shapes=[pltpu.VMEM(shape, jnp.float32), pltpu.SemaphoreType.DMA((peers,))],
        compiler_params=pltpu.CompilerParams(vmem_limit_bytes=8 * 1024 * 1024),
        name="pack_step",
    )(picked, returned, base, live)


def place_kernel(slots, half, received, out, weights, estimate, moved, gone):
    sums = received[0, 100:101, :]
    for peer in range(1, received.shape[0]):
        sums = sums + received[peer, 100:101, :]
    sums = jnp.broadcast_to(sums, (8, BLK))
    ratio = sums / pltpu.roll(sums, BLK - 8, axis=1)
    lane = lax.broadcasted_iota(jnp.int32, (8, BLK), 1)
    reference = jnp.sum(jnp.where(lane == 0, ratio, 0.0), axis=1, keepdims=True)[0:1, :]
    own = jnp.where(half[0] == 0, ratio, pltpu.roll(ratio, BLK - 4, axis=1))
    estimate[...] = own[0:1, 0:4]
    copies, step = [], weights.shape[0] // 4
    for d in range(weights.shape[0]):
        peer, k = slots[d] // CAP, slots[d] % CAP
        for c in range(3):
            at = pl.multiple_of(k * 24 + c * 8, 8)
            moved[c, :, d * BLK : (d + 1) * BLK] = received[peer, pl.ds(at, 8), :]
        level = received[peer, pl.ds(96 + k, 1), :]
        weights[d : d + 1, :] = jnp.exp(-(level - reference))
        if (d + 1) % step == 0:
            part = pl.ds((d + 1 - step) * BLK, step * BLK)
            copies.append(
                pltpu.make_async_copy(
                    moved.at[:, :, part], out.at[:, :, part], gone.at[len(copies)]
                )
            )
            copies[-1].start()
    for copy in copies:
        copy.wait()


def place_step(slots, half, received):
    vmem = pl.BlockSpec(memory_space=pltpu.VMEM)
    smem = pl.BlockSpec(memory_space=pltpu.SMEM)
    blocks = slots.shape[0]
    return pl.pallas_call(
        place_kernel,
        out_shape=(
            jax.ShapeDtypeStruct((3, 8, blocks * BLK), jnp.float32),
            jax.ShapeDtypeStruct((blocks, BLK), jnp.float32),
            jax.ShapeDtypeStruct((1, NG // 2), jnp.float32),
        ),
        in_specs=[smem, smem, vmem],
        out_specs=(pl.BlockSpec(memory_space=pltpu.HBM), vmem, vmem),
        scratch_shapes=[
            pltpu.VMEM((3, 8, blocks * BLK), jnp.float32),
            pltpu.SemaphoreType.DMA((4,)),
        ],
        compiler_params=pltpu.CompilerParams(vmem_limit_bytes=8 * 1024 * 1024),
        name="place_step",
    )(slots, half, received)


def nuclear_repulsion(centers, charges):
    offsets = centers[:, :, None, :] - centers[:, None, :, :]
    identity = jnp.eye(NA, dtype=jnp.float32)
    distance = jnp.sqrt(jnp.sum(offsets * offsets, axis=3) + identity)
    product = charges[:, None] * charges[None, :] * (1.0 - identity)
    return 0.5 * jnp.sum(product / distance, axis=(1, 2))


def nucleus_tables(centers, charges, decay, coefficients):
    c = jnp.moveaxis(centers, 1, 0)
    k = (decay * LOG2E)[:, None]
    k2 = k * k
    scale = decay[:, None] * k
    ones = jnp.ones((NA, NG), jnp.float32)

    def thirds(x):
        high = lax.reduce_precision(x, 8, 7)
        rest = x - high
        middle = lax.reduce_precision(rest, 8, 7)
        return high, middle, rest - middle

    rows = []
    for value in [-2.0 * k2 * c[:, :, d] for d in range(3)] + [k2 * ones]:
        high, middle, low = thirds(value)
        rows += [high, middle, low, high, middle, high]
    rows += list(thirds(k2 * (jnp.sum(c * c, axis=2) + SOFT)))
    rows += [jnp.zeros_like(ones)] * (2 * BLK // 8 - len(rows))
    spread = jnp.stack(rows, axis=-1).reshape(NA * NG, len(rows), 1)
    spread = jnp.broadcast_to(spread, (NA * NG, len(rows), 8)).reshape(NA * NG, 2 * BLK)

    factors = [
        jnp.log2(coefficients[:, None] * scale) * ones,
        ones / scale,
        (0.5 * SOFT) * k2 * ones,
        c[:, :, 0],
        c[:, :, 1],
        c[:, :, 2],
        (charges[:, None] * k) * ones,
    ]
    table = jnp.broadcast_to(jnp.stack(factors)[..., None], (len(factors), NA, NG, BLK))
    return spread, table


def by_blocks(x):
    e, c, w = x.shape
    return x.reshape(e, c, w // BLK, BLK).transpose(2, 1, 0, 3).reshape(w // BLK, c * e, BLK)


def local(
    positions,
    diffusion_noise,
    base_nuclei,
    displacements,
    charges,
    orbital_decay,
    coefficients,
    weights,
    counts,
    branch_source,
):
    blocks_here = counts.shape[0]
    peers = lax.axis_size(GX)
    replica = lax.axis_index("gz")
    member = lax.axis_index(GZY)
    device = lax.axis_index(GX)

    sent = by_blocks(positions)
    whole = lax.all_to_all(sent.reshape(EB, 2, 24, BLK), GZY, 0, 0, tiled=True)

    base = sent + STEP_ROOT * by_blocks(diffusion_noise)
    centers = base_nuclei[None, :, :] + displacements
    spread, table = nucleus_tables(centers, charges, orbital_decay, coefficients)
    nuclear = jnp.broadcast_to(nuclear_repulsion(centers, charges)[:, None], (NG, BLK))
    live = jnp.where(
        jnp.arange(BLK, dtype=jnp.int32)[None, :] < counts[:, None],
        weights.reshape(blocks_here, BLK),
        0.0,
    )
    own_live = lax.dynamic_slice_in_dim(live, member * 2, 2, 0)

    block_range = jnp.arange(blocks_here, dtype=jnp.int32)
    total = branch_source.shape[0]
    own_ids = device * blocks_here + block_range
    matches = (branch_source[None, :] == own_ids[:, None]).astype(jnp.int32)
    dest_slot = jnp.sum(matches * jnp.arange(total, dtype=jnp.int32)[None, :], axis=1)
    dest_device = dest_slot // blocks_here
    earlier = (
        (dest_device[None, :] == dest_device[:, None]) & (dest_slot[None, :] < dest_slot[:, None])
    ).astype(jnp.int32)
    send_slot = dest_device * CAP + jnp.sum(earlier, axis=1)
    selection = (
        jnp.arange(peers * CAP, dtype=jnp.int32)[:, None] == send_slot[None, :]
    ).astype(jnp.int32)
    picked = jnp.sum(selection * block_range[None, :], axis=1)
    my_sources = lax.dynamic_slice_in_dim(branch_source, device * blocks_here, blocks_here, 0)
    source_device = my_sources // blocks_here
    before = (
        (source_device[None, :] == source_device[:, None])
        & (block_range[None, :] < block_range[:, None])
    ).astype(jnp.int32)
    slots = source_device * CAP + jnp.sum(before, axis=1)

    out = walker_step(whole, spread, table, nuclear, own_live)
    returned = lax.all_to_all(out, GZY, 0, 0, tiled=True).reshape(blocks_here, 32, BLK)
    send, local_energy = pack_step(picked, returned, base, live, peers)
    received = lax.all_to_all(send, GX, 0, 0, tiled=True)
    moved, new_weights, estimate = place_step(slots, replica.reshape(1), received)
    return (local_energy, estimate.reshape(NG // 2), moved.transpose(1, 0, 2), new_weights.reshape(blocks_here * BLK))


def solution(mesh):
    split = Mesh(
        mesh.devices.reshape(mesh.shape["gz"], 4, 4, mesh.shape["gy"]), ("gz", "gx_0", "gx_1", "gy")
    )
    placed = (
        P(("gz", "gy"), None, GX),
        P(("gz", "gy"), None, GX),
        P(),
        P(),
        P(),
        P(),
        P(),
        P(GX),
        P(GX),
        P(),
    )
    return jax.shard_map(
        local,
        mesh=split,
        in_specs=placed,
        out_specs=(P("gz", GX), P("gz"), P(("gz", "gy"), None, GX), P(GX)),
        check_vma=False,
    )
```

```python
import functools
import math

import jax
import jax.numpy as jnp
from jax import lax
from jax.experimental import pallas as pl
from jax.experimental.pallas import tpu as pltpu
from jax.sharding import Mesh
from jax.sharding import PartitionSpec as P

NE = 128
NA = 16
NG = 8
BLK = 128
EB = 16
GROUP = 4
CAP = 4
SLOT_ROWS = 24
PEER_ROWS = CAP * SLOT_ROWS + 8
GX = ("gx_0", "gx_1")
GZY = ("gz", "gy")

SOFT = 0.04
TIME_STEP = 0.01
STEP_ROOT = 0.1
LN2 = math.log(2.0)
LOG2E = 1.0 / LN2

def roll8(x, shift):
    shift %= 8
    return x if shift == 0 else pltpu.roll(x, shift, axis=0)


def pair_part(pos, rot, back, grad):
    zero = jnp.zeros((8, BLK), jnp.float32)

    def prepare(p, _):
        for h in range(2):
            for c in range(3):
                x = pos[p, h, c * 8 : c * 8 + 8, :]
                for s in range(1, 8):
                    rot[p, h, s - 1, c * 8 : c * 8 + 8, :] = roll8(x, -s)
        return 0

    lax.fori_loop(0, EB, prepare, 0)

    def terms(xi, xj, sums, half):
        d = [xi[c] - xj[c] for c in range(3)]
        square = (d[0] * d[0] + d[1] * d[1]) + (d[2] * d[2] + SOFT)
        inv = lax.rsqrt(square)
        p = 1.0 / (square * inv + 1.0)
        p2 = p * p
        slope = p2 * inv
        parts = (inv, slope, p2 * p, (inv * inv) * inv)
        if half:
            parts = tuple(0.5 * part for part in parts)
        return [slope * d[c] for c in range(3)], tuple(a + b for a, b in zip(sums, parts))

    def load3(ref, *at):
        return [ref[(*at, slice(c * 8, c * 8 + 8), slice(None))] for c in range(3)]

    def store3(ref, values, *at):
        for c in range(3):
            ref[(*at, slice(c * 8, c * 8 + 8), slice(None))] = values[c]

    def turned(j, h, s):
        return load3(pos, j, h) if s == 0 else load3(rot, j, h, s - 1)

    def block_pair(i, j, h, xi, gi, sums, fresh=()):
        for s in range(8):
            f, sums = terms(xi, turned(j, h, s), sums, False)
            gi = [gi[c] + f[c] for c in range(3)]
            if s not in fresh:
                b = load3(back, j, h, s)
                f = [b[c] + f[c] for c in range(3)]
            store3(back, f, j, h, s)
        return gi, sums

    def inside(t, sums):
        out = []
        untouched = (0, 4, 5, 6, 7)
        for h in range(2):
            acc = sums[h]
            own = []
            for i in (2 * t, 2 * t + 1):
                xi, gi = load3(pos, i, h), [zero] * 3
                for s in range(1, 5):
                    f, acc = terms(xi, turned(i, h, s), acc, s == 4)
                    gi = [gi[c] + f[c] for c in range(3)]
                    if s < 4:
                        store3(back, f, i, h, s)
                own.append(gi)
            i, j = 2 * t, 2 * t + 1
            for s in untouched:
                store3(back, [zero] * 3, i, h, s)
            gi, acc = block_pair(i, j, h, load3(pos, i, h), own[0], acc, untouched)
            store3(grad, gi, i, h)
            store3(grad, own[1], j, h)
            out.append(acc)
        return tuple(out)

    def across(u, t, sums):
        out = []
        for h in range(2):
            acc = sums[h]
            for i in (2 * u, 2 * u + 1):
                xi, gi = load3(pos, i, h), load3(grad, i, h)
                for j in (2 * t, 2 * t + 1):
                    gi, acc = block_pair(i, j, h, xi, gi, acc)
                store3(grad, gi, i, h)
            out.append(acc)
        return tuple(out)

    def outer(t, sums):
        sums = inside(t, sums)
        return lax.fori_loop(0, t, lambda u, carry: across(u, t, carry), sums)

    start = ((zero,) * 4, (zero,) * 4)
    sums = lax.fori_loop(0, EB // 2, outer, start)

    def finish(p, squares):
        out = []
        for h in range(2):
            acc = squares[h]
            for c in range(3):
                g = grad[p, h, c * 8 : c * 8 + 8, :]
                for s in range(8):
                    g = g - roll8(back[p, h, s, c * 8 : c * 8 + 8, :], s)
                g = 0.5 * g
                grad[p, h, c * 8 : c * 8 + 8, :] = g
                acc = acc + g * g
            out.append(acc)
        return tuple(out)

    squares = lax.fori_loop(0, EB, finish, (zero, zero))
    totals = []
    for h in range(2):
        inv, slope, cube, inv3 = sums[h]
        t = inv - (1.0 - 1.5 * SOFT) * slope + (1.0 - SOFT) * cube - (0.5 * SOFT) * inv3
        t = t - 0.5 * squares[h]
        totals.append(jnp.broadcast_to(jnp.sum(t, axis=0, keepdims=True), (8, BLK)))
    return totals


def split3(x):
    high = x.astype(jnp.bfloat16).astype(jnp.float32)
    rest = x - high
    middle = rest.astype(jnp.bfloat16).astype(jnp.float32)
    return high, middle, rest - middle


def walker_kernel(
    pos, spread, table, nuclear, live, out,
    rot, back, grad, left, right, square0, square1, reaches, firsts,
):
    totals = pair_part(pos, rot, back, grad)
    zero = jnp.zeros((8, BLK), jnp.float32)

    column = lax.broadcasted_iota(jnp.int32, (8 * NA, 2 * BLK), 1)
    for e in range(8):
        weights = jnp.where(column % 8 == e, spread[...], 0.0)
        left[e * 128 : e * 128 + 128, :] = weights.astype(jnp.bfloat16)
    for row in range(24, 32):
        right[row * 8 : row * 8 + 8, :] = jnp.full((8, 2 * BLK), 1.0 if row < 27 else 0.0)

    def features(p):
        for h in range(2):
            lanes = slice(h * BLK, h * BLK + BLK)
            x = [pos[p, h, c * 8 : c * 8 + 8, :] for c in range(3)]
            x.append(x[0] * x[0] + x[1] * x[1] + x[2] * x[2])
            tiles = []
            for value in x:
                high, middle, low = split3(value)
                tiles += [high, high, high, middle, middle, low]
            for row, tile in enumerate(tiles):
                right[row * 8 : row * 8 + 8, lanes] = tile

    def squares(square, first, count):
        rows = slice(first * 128, (first + count) * 128)
        factor = right[...].astype(jnp.bfloat16)
        square[rows, :] = jnp.dot(left[rows, :], factor, preferred_element_type=jnp.float32)

    def orbitals(p, square, carry, first):
        energy, logs, pots = (list(part) for part in carry)
        group = range(first, first + GROUP)
        acc = {(e, h): [zero] * 7 for e in group for h in range(2)}
        for a in range(NA):
            level, share, soft, cx, cy, cz, charge = (table[k, a] for k in range(7))
            for h in range(2):
                lanes = slice(h * BLK, h * BLK + BLK)
                near = []
                for e in group:
                    at = (e * NA + a) * 8
                    sq = square[at : at + 8, lanes]
                    inv = lax.rsqrt(sq)
                    amp = jnp.exp2(level - sq * inv)
                    u = amp * inv
                    s = acc[e, h]
                    acc[e, h] = [
                        s[0] + amp * share,
                        s[1] + amp,
                        s[2] + (u * inv) * ((inv + LN2) * soft),
                        s[3] + u,
                        s[4] + u * cx,
                        s[5] + u * cy,
                        s[6] + u * cz,
                    ]
                    near.append(inv)
                pots[h] = pots[h] + functools.reduce(jnp.add, near) * charge
        for e in group:
            for h in range(2):
                phi, amps, soft, us = acc[e, h][:4]
                u = acc[e, h][4:]
                ratio = 1.0 / phi
                at = [slice(c * 8 + e, c * 8 + e + 1) for c in range(3)]
                j = [jnp.broadcast_to(grad[p, h, at[c], :], (8, BLK)) for c in range(3)]
                reach = jnp.broadcast_to(reaches[p, h, e : e + 1, :], (8, BLK))
                part = (0.5 * LN2) * amps - soft - us * reach
                part = part + (u[0] * j[0] + u[1] * j[1] + u[2] * j[2])
                energy[h] = energy[h] - part * ratio
                logs[h] = logs[h] + jnp.log2(phi)
                for k, value in enumerate((*u, us, ratio)):
                    firsts[h, k, e : e + 1, :] = value[0:1, :]
        return tuple(energy), tuple(logs), tuple(pots)

    def reaching(p, _):
        for h in range(2):
            dots = [
                pos[p, h, c * 8 : c * 8 + 8, :] * grad[p, h, c * 8 : c * 8 + 8, :] for c in range(3)
            ]
            reaches[p, h] = (1.0 + dots[0]) + (dots[1] + dots[2])
        return 0

    lax.fori_loop(0, EB, reaching, 0)

    def drift(p):
        for h in range(2):
            for c in range(3):
                rows = slice(c * 8, c * 8 + 8)
                own = (firsts[h, c] - pos[p, h, rows, :] * firsts[h, 3]) * firsts[h, 4]
                out[p, h, rows, :] = own + grad[p, h, rows, :]

    features(0)
    squares(square0, 0, 8)

    def one_block(p, now, later, carry):
        features(jnp.minimum(p + 1, EB - 1))
        for first in range(0, 8, GROUP):
            squares(later, first, GROUP)
            carry = orbitals(p, now, carry, first)
        drift(p)
        return carry

    def some_blocks(t, carry):
        for k in range(0, 4, 2):
            carry = one_block(4 * t + k, square0, square1, carry)
            carry = one_block(4 * t + k + 1, square1, square0, carry)
        return carry

    energy, logs, pots = lax.fori_loop(
        0, EB // 4, some_blocks, ((zero, zero), (zero, zero), (zero, zero))
    )
    row = lax.broadcasted_iota(jnp.int32, (8, BLK), 0)
    lane = lax.broadcasted_iota(jnp.int32, (8, BLK), 1)
    numerator = jnp.zeros((8, 1), jnp.float32)
    denominator = jnp.zeros((8, 1), jnp.float32)
    local = []
    for h in range(2):
        e = (energy[h] - pots[h] + totals[h] + nuclear[...]) * (1.0 / NE)
        weight = jnp.exp2(2.0 * (logs[h] - jnp.broadcast_to(logs[h][0:1, :], (8, BLK))))
        weight = weight * jnp.broadcast_to(live[h : h + 1, :], (8, BLK))
        numerator = numerator + jnp.sum(weight * e, axis=1, keepdims=True)
        denominator = denominator + jnp.sum(weight, axis=1, keepdims=True)
        local.append(e)
    placed = jnp.where(lane == row, numerator, 0.0) + jnp.where(lane == row + 8, denominator, 0.0)
    placed = jnp.broadcast_to(jnp.sum(placed, axis=0, keepdims=True), (8, BLK))
    for h in range(2):
        first = jnp.broadcast_to(local[h][0:1, :], (8, BLK))
        for half in range(2):
            e = local[h] if half == 0 else roll8(local[h], 4)
            tile = jnp.where(row < 4, e, jnp.where(row == 4, first, placed))
            for q in range(8):
                out[half * 8 + q, h, 24:32, :] = tile


def walker_step(whole, spread, table, nuclear, live):
    vmem = pl.BlockSpec(memory_space=pltpu.VMEM)
    rows, width = 8 * NA * 8, 2 * BLK
    return pl.pallas_call(
        walker_kernel,
        out_shape=jax.ShapeDtypeStruct((EB, 2, 32, BLK), jnp.float32),
        in_specs=[vmem] * 5,
        out_specs=vmem,
        scratch_shapes=[
            pltpu.VMEM((EB, 2, 7, 24, BLK), jnp.float32),
            pltpu.VMEM((EB, 2, 8, 24, BLK), jnp.float32),
            pltpu.VMEM((EB, 2, 24, BLK), jnp.float32),
            pltpu.VMEM((rows, width), jnp.bfloat16),
            pltpu.VMEM((width, width), jnp.float32),
            pltpu.VMEM((rows, width), jnp.float32),
            pltpu.VMEM((rows, width), jnp.float32),
            pltpu.VMEM((EB, 2, 8, BLK), jnp.float32),
            pltpu.VMEM((2, 5, 8, BLK), jnp.float32),
        ],
        compiler_params=pltpu.CompilerParams(vmem_limit_bytes=24 * 1024 * 1024),
        name="walker_step",
    )(whole, spread, table, nuclear, live)


def pack_kernel(picked, returned, base, live, send, energy):
    sums = returned[0, 29:30, :]
    for p in range(1, EB):
        sums = sums + returned[2 * p, 29:30, :]
    for b in range(2 * EB):
        energy[:, b * BLK : (b + 1) * BLK] = returned[b, 24:28, :]

    def one_peer(peer, _):
        for k in range(CAP):
            b = picked[peer * CAP + k]
            for c in range(3):
                send[peer, k * 24 + c * 8 : k * 24 + c * 8 + 8, :] = (
                    base[b, c * 8 : c * 8 + 8, :] + TIME_STEP * returned[b, c * 8 : c * 8 + 8, :]
                )
            alive = live[pl.ds(b, 1), :]
            level = returned[b, 28:29, :] - jnp.log(alive)
            send[peer, 96 + k : 97 + k, :] = jnp.where(alive > 0.0, level, 3.0e38)
        send[peer, 100:101, :] = sums
        send[peer, 101:104, :] = jnp.zeros((3, BLK), jnp.float32)
        return 0

    lax.fori_loop(0, send.shape[0], one_peer, 0)


def pack_step(picked, returned, base, live, peers):
    vmem = pl.BlockSpec(memory_space=pltpu.VMEM)
    return pl.pallas_call(
        pack_kernel,
        out_shape=(
            jax.ShapeDtypeStruct((peers, PEER_ROWS, BLK), jnp.float32),
            jax.ShapeDtypeStruct((NG // 2, 2 * EB * BLK), jnp.float32),
        ),
        in_specs=[pl.BlockSpec(memory_space=pltpu.SMEM)] + [vmem] * 3,
        out_specs=(vmem, vmem),
        compiler_params=pltpu.CompilerParams(vmem_limit_bytes=8 * 1024 * 1024),
        name="pack_step",
    )(picked, returned, base, live)


def place_kernel(slots, half, received, moved, weights, estimate):
    sums = received[0, 100:101, :]
    for peer in range(1, received.shape[0]):
        sums = sums + received[peer, 100:101, :]
    sums = jnp.broadcast_to(sums, (8, BLK))
    ratio = sums / pltpu.roll(sums, BLK - 8, axis=1)
    lane = lax.broadcasted_iota(jnp.int32, (8, BLK), 1)
    reference = jnp.sum(jnp.where(lane == 0, ratio, 0.0), axis=1, keepdims=True)[0:1, :]
    own = jnp.where(half[0] == 0, ratio, pltpu.roll(ratio, BLK - 4, axis=1))
    estimate[...] = own[0:1, 0:4]
    for d in range(weights.shape[0]):
        peer, k = slots[d] // CAP, slots[d] % CAP
        for c in range(3):
            at = pl.multiple_of(k * 24 + c * 8, 8)
            moved[c, :, d * BLK : (d + 1) * BLK] = received[peer, pl.ds(at, 8), :]
        level = received[peer, pl.ds(96 + k, 1), :]
        weights[d : d + 1, :] = jnp.exp(-(level - reference))


def place_step(slots, half, received):
    vmem = pl.BlockSpec(memory_space=pltpu.VMEM)
    smem = pl.BlockSpec(memory_space=pltpu.SMEM)
    blocks = slots.shape[0]
    return pl.pallas_call(
        place_kernel,
        out_shape=(
            jax.ShapeDtypeStruct((3, 8, blocks * BLK), jnp.float32),
            jax.ShapeDtypeStruct((blocks, BLK), jnp.float32),
            jax.ShapeDtypeStruct((1, NG // 2), jnp.float32),
        ),
        in_specs=[smem, smem, vmem],
        out_specs=(vmem, vmem, vmem),
        compiler_params=pltpu.CompilerParams(vmem_limit_bytes=8 * 1024 * 1024),
        name="place_step",
    )(slots, half, received)


def nuclear_repulsion(centers, charges):
    offsets = centers[:, :, None, :] - centers[:, None, :, :]
    identity = jnp.eye(NA, dtype=jnp.float32)
    distance = jnp.sqrt(jnp.sum(offsets * offsets, axis=3) + identity)
    product = charges[:, None] * charges[None, :] * (1.0 - identity)
    return 0.5 * jnp.sum(product / distance, axis=(1, 2))


def nucleus_tables(centers, charges, decay, coefficients):
    c = jnp.moveaxis(centers, 1, 0)
    k = (decay * LOG2E)[:, None]
    k2 = k * k
    scale = decay[:, None] * k
    ones = jnp.ones((NA, NG), jnp.float32)

    def thirds(x):
        high = lax.reduce_precision(x, 8, 7)
        rest = x - high
        middle = lax.reduce_precision(rest, 8, 7)
        return high, middle, rest - middle

    rows = []
    for value in [-2.0 * k2 * c[:, :, d] for d in range(3)] + [k2 * ones]:
        high, middle, low = thirds(value)
        rows += [high, middle, low, high, middle, high]
    rows += list(thirds(k2 * (jnp.sum(c * c, axis=2) + SOFT)))
    rows += [jnp.zeros_like(ones)] * (2 * BLK // 8 - len(rows))
    spread = jnp.stack(rows, axis=-1).reshape(NA * NG, len(rows), 1)
    spread = jnp.broadcast_to(spread, (NA * NG, len(rows), 8)).reshape(NA * NG, 2 * BLK)

    factors = [
        jnp.log2(coefficients[:, None] * scale) * ones,
        ones / scale,
        (0.5 * SOFT) * k2 * ones,
        c[:, :, 0],
        c[:, :, 1],
        c[:, :, 2],
        (charges[:, None] * k) * ones,
    ]
    table = jnp.broadcast_to(jnp.stack(factors)[..., None], (len(factors), NA, NG, BLK))
    return spread, table


def by_blocks(x):
    e, c, w = x.shape
    return x.reshape(e, c, w // BLK, BLK).transpose(2, 1, 0, 3).reshape(w // BLK, c * e, BLK)


def local(
    positions,
    diffusion_noise,
    base_nuclei,
    displacements,
    charges,
    orbital_decay,
    coefficients,
    weights,
    counts,
    branch_source,
):
    blocks_here = counts.shape[0]
    peers = lax.axis_size(GX)
    replica = lax.axis_index("gz")
    member = lax.axis_index(GZY)
    device = lax.axis_index(GX)

    sent = by_blocks(positions)
    whole = lax.all_to_all(sent.reshape(EB, 2, 24, BLK), GZY, 0, 0, tiled=True)

    base = sent + STEP_ROOT * by_blocks(diffusion_noise)
    centers = base_nuclei[None, :, :] + displacements
    spread, table = nucleus_tables(centers, charges, orbital_decay, coefficients)
    nuclear = jnp.broadcast_to(nuclear_repulsion(centers, charges)[:, None], (NG, BLK))
    live = jnp.where(
        jnp.arange(BLK, dtype=jnp.int32)[None, :] < counts[:, None],
        weights.reshape(blocks_here, BLK),
        0.0,
    )
    own_live = lax.dynamic_slice_in_dim(live, member * 2, 2, 0)

    block_range = jnp.arange(blocks_here, dtype=jnp.int32)
    total = branch_source.shape[0]
    own_ids = device * blocks_here + block_range
    matches = (branch_source[None, :] == own_ids[:, None]).astype(jnp.int32)
    dest_slot = jnp.sum(matches * jnp.arange(total, dtype=jnp.int32)[None, :], axis=1)
    dest_device = dest_slot // blocks_here
    earlier = (
        (dest_device[None, :] == dest_device[:, None]) & (dest_slot[None, :] < dest_slot[:, None])
    ).astype(jnp.int32)
    send_slot = dest_device * CAP + jnp.sum(earlier, axis=1)
    selection = (
        jnp.arange(peers * CAP, dtype=jnp.int32)[:, None] == send_slot[None, :]
    ).astype(jnp.int32)
    picked = jnp.sum(selection * block_range[None, :], axis=1)
    my_sources = lax.dynamic_slice_in_dim(branch_source, device * blocks_here, blocks_here, 0)
    source_device = my_sources // blocks_here
    before = (
        (source_device[None, :] == source_device[:, None])
        & (block_range[None, :] < block_range[:, None])
    ).astype(jnp.int32)
    slots = source_device * CAP + jnp.sum(before, axis=1)

    out = walker_step(whole, spread, table, nuclear, own_live)
    returned = lax.all_to_all(out, GZY, 0, 0, tiled=True).reshape(blocks_here, 32, BLK)
    send, local_energy = pack_step(picked, returned, base, live, peers)
    received = lax.all_to_all(send, GX, 0, 0, tiled=True)
    moved, new_weights, estimate = place_step(slots, replica.reshape(1), received)
    return (local_energy, estimate.reshape(NG // 2), moved.transpose(1, 0, 2), new_weights.reshape(blocks_here * BLK))


def solution(mesh):
    split = Mesh(
        mesh.devices.reshape(mesh.shape["gz"], 4, 4, mesh.shape["gy"]), ("gz", "gx_0", "gx_1", "gy")
    )
    placed = (
        P(("gz", "gy"), None, GX),
        P(("gz", "gy"), None, GX),
        P(),
        P(),
        P(),
        P(),
        P(),
        P(GX),
        P(GX),
        P(),
    )
    return jax.shard_map(
        local,
        mesh=split,
        in_specs=placed,
        out_specs=(P("gz", GX), P("gz"), P(("gz", "gy"), None, GX), P(GX)),
        check_vma=False,
    )
```
